32 devices in a mesh: groups: 1, expert: 16 (over z, y, x), replica: 2 (over core).
Axes of the slice: x: 2, y: 2, z: 4, core: 2. Of those that a mesh axis runs over, the one named last changes fastest.
Arguments:
- queries: bfloat16 [128, 8192], P(('groups', 'expert', 'replica')), may hold values from -250 to 250
- token_keys: bfloat16 [128, 512], P(('groups', 'expert', 'replica')), may hold values from -6 to 6
- token_values: bfloat16 [128, 512], P(('groups', 'expert', 'replica')), may hold values from -6 to 6
- stored_keys: bfloat16 [128, 256, 512], P(('groups', 'expert', 'replica')), may hold values from -7 to 7
- stored_values: bfloat16 [128, 256, 512], P(('groups', 'expert', 'replica')), may hold values from -6 to 6
- kv_len: int32 [128], P(('groups', 'expert', 'replica')), may hold values from 2 to 256, as said below
- residual: bfloat16 [128, 4096], P(('groups', 'expert', 'replica')), may hold values from -6 to 6
- out_weight: bfloat16 [8192, 4096], P(('expert', 'replica')), may hold values from -0.1875 to 0.1875
- norm_gain: bfloat16 [4096], replicated, may hold values from 0.25 to 1.75
- expert_ids: int32 [128, 8], P(('groups', 'expert')), may hold values from 0 to 15, all different within a row; in each aligned block of 8 rows (0 to 7, 8 to 15, ...) at most 4 rows name the same one
- route_weight: float32 [128, 8], P(('groups', 'expert')), may hold values from 0.05 to 1
- w_gate: bfloat16 [16, 4096, 768], P('expert', None, 'replica'), may hold values from -0.09375 to 0.09375
- w_up: bfloat16 [16, 4096, 768], P('expert', None, 'replica'), may hold values from -0.09375 to 0.09375
- w_down: bfloat16 [16, 768, 4096], P('expert', 'replica'), may hold values from -0.4375 to 0.4375
Outputs:
- updated: bfloat16 [128, 4096], P(('groups', 'expert', 'replica'))
The draws below stay inside these ranges and needn't reach their ends.
Inputs may be any that keep to these rules, and one draw needn't show every extreme that they name: `kv_len`: at least 2; some sequence uses all 256 positions. `expert_ids`: each token names 8 different experts; in each aligned block of 8 tokens no expert is named by more than 4 tokens, and some block reaches it.
All inputs are finite; a program needn't handle non-finite values.
Results may differ from the reference program's by a relative error of at most 0.01.
Values may be sent and summed in bfloat16 or wider, within the bound.
A program may use at most 64 MiB of HBM per device.

```python
import math
import jax
import jax.numpy as jnp
import numpy as np
from jax import lax

D = 4096
QUERY_HEADS = 64
KEY_VALUE_HEADS = 4
HEAD_WIDTH = 128
FF = 768
TOPK = 8
SEQ_DEV = 4
CACHE_POSITIONS = 256
EXPERTS = 16
SEQUENCE_TOTAL = 128
MOST = 4
N_EXPERT = 16
N_REPLICA = 2


def key_lookup(key):
    return jnp.clip(jax.random.normal(jax.random.fold_in(key, 11), (SEQUENCE_TOTAL, CACHE_POSITIONS, KEY_VALUE_HEADS * HEAD_WIDTH), jnp.float32), -6.0, 6.0)


def draw_queries(key, part):
    base = jnp.clip(jax.random.normal(jax.random.fold_in(key, 5), (SEQUENCE_TOTAL, QUERY_HEADS * HEAD_WIDTH), jnp.float32), -6.0, 6.0)
    return base.astype(jnp.bfloat16)


def draw_stored_keys(key, part):
    table = key_lookup(key)
    return table.astype(jnp.bfloat16)


def draw_kv_len(key, part):
    lengths = jax.random.randint(jax.random.fold_in(key, 3), (SEQUENCE_TOTAL,), 2, CACHE_POSITIONS + 1, jnp.int32)
    chosen = jax.random.randint(jax.random.fold_in(key, 4), (), 0, SEQUENCE_TOTAL, jnp.int32)
    return jnp.where(jnp.arange(SEQUENCE_TOTAL, dtype=jnp.int32) == chosen, CACHE_POSITIONS, lengths).astype(jnp.int32)


def shard_levels(own_key, shape, cuts, least, high):
    gain, own = 1.0, jax.random.fold_in(own_key, 6)
    for dim, parts in cuts:
        heights = jnp.exp(jax.random.uniform(jax.random.fold_in(own, dim), (parts,), jnp.float32, least / len(cuts), high / len(cuts)))
        gain = gain * jnp.repeat(heights, shape[dim] // parts).reshape([-1 if axis == dim else 1 for axis in range(len(shape))])
    return gain


def shared_out(own_key, own, number, rows, number_of, top, most, slope):
    ranking = jax.random.permutation(own_key, number_of)
    heavy_load, common = portions_of(number_of, rows * top, most, slope, True), portions_of(number_of, rows * top, most, slope, False)
    places = jnp.arange(number_of)

    def named(tallies, turn):
        used = int((tallies > 0).sum())
        fixed = max(1, used // 4)
        shifted = fixed + (places - fixed + turn * (used - fixed)) % max(1, number_of - fixed)
        return jnp.zeros((number_of,), jnp.int32).at[ranking[jnp.where(places < fixed, places, shifted)]].set(jnp.asarray(tallies, jnp.int32))

    tallies = jnp.where(number % 4 == 0, named(heavy_load, number // 4), named(common, number - number // 4 - 1))
    mixed = jax.random.permutation(jax.random.fold_in(own, 3), number_of)
    donor, receiver = mixed[0:number_of // 2 * 2:2], mixed[1:number_of // 2 * 2:2]
    margin = jnp.minimum(tallies[donor] - 1, most - tallies[receiver]) // 2
    margin = jnp.where((donor == ranking[0]) | (receiver == ranking[0]) | (tallies[receiver] == 0), 0, jnp.maximum(margin, 0))
    shifted = jax.random.randint(jax.random.fold_in(own, 4), (number_of // 2,), 0, 1 << 20) % (margin + 1)
    tallies = tallies.at[donor].add(-shifted).at[receiver].add(shifted)
    items = jnp.searchsorted(jnp.cumsum(tallies), jnp.arange(rows * top), side="right").astype(jnp.int32)
    listing = items.reshape(top, rows).T
    listing = listing[jax.random.permutation(jax.random.fold_in(own, 1), rows)]
    turn = jax.random.randint(jax.random.fold_in(own, 2), (rows, 1), 0, top)
    return jnp.take_along_axis(listing, (jnp.arange(top)[None, :] + turn) % top, axis=1)


def portions_of(number_of, total, limit, lean, full):
    portions = [(1 << 20) // math.isqrt(grade ** lean) + 1 for grade in range(1, number_of + 1)]
    largest = limit if full else min(limit, max(-(-total // number_of), total * portions[0] // sum(portions)))
    least = 1 if total - largest >= number_of - 1 else 0
    given, rest = [largest] + [least] * (number_of - 1), total - largest - least * (number_of - 1)
    while rest > 0:
        movable = [i for i in range(1, number_of) if given[i] < largest] or [i for i in range(1, number_of) if given[i] < limit]
        whole, remaining = sum([portions[i] for i in movable]), rest
        for i in movable:
            addition = min(limit - given[i], max(1, remaining * portions[i] // whole), rest)
            given[i] = given[i] + addition
            rest = rest - addition
    return np.array(given)


def normal_values(key, shape, width, reach, pieces=(), held_as=jnp.bfloat16):
    entries = width * jax.random.normal(key, shape, jnp.float32)
    if pieces:
        entries = entries * shard_levels(key, shape, pieces, -0.22, 0.18)
    return jnp.clip(entries, -reach, reach).astype(held_as)


def setup_inputs(seed: int = 0, part: int = 0) -> dict:
    key_list = jax.random.split(jax.random.key(seed), 15)
    part_splits = jax.random.split(jax.random.fold_in(key_list[14], part), 15)
    queries = draw_queries(jax.random.fold_in(jax.random.fold_in(key_list[14], part), 71), part)
    token_keys = normal_values(part_splits[1], (SEQUENCE_TOTAL, KEY_VALUE_HEADS * HEAD_WIDTH), 1.0, 6.0, ((0, 32),))
    token_values = normal_values(part_splits[2], (SEQUENCE_TOTAL, KEY_VALUE_HEADS * HEAD_WIDTH), 1.0, 6.0, ((0, 32),))
    stored_keys = draw_stored_keys(jax.random.fold_in(jax.random.fold_in(key_list[14], part), 71), part)
    stored_values = normal_values(part_splits[4], (SEQUENCE_TOTAL, CACHE_POSITIONS, KEY_VALUE_HEADS * HEAD_WIDTH), 1.0, 6.0, ((0, 32),))
    kv_len = draw_kv_len(jax.random.fold_in(jax.random.fold_in(key_list[14], part), 71), part)
    residual = normal_values(part_splits[6], (SEQUENCE_TOTAL, D), 1.0, 6.0, ((0, 32),))
    out_weight = normal_values(key_list[7], (QUERY_HEADS * HEAD_WIDTH, D), (QUERY_HEADS * HEAD_WIDTH // 8) ** -0.5, 0.1875, ((0, 32),))
    norm_gain = jnp.clip(1.0 + 0.15 * jax.random.normal(key_list[8], (D,), jnp.float32), 0.25, 1.75).astype(jnp.bfloat16)
    expert_ids_keys = jax.random.split(jax.random.fold_in(part_splits[9], 1), SEQUENCE_TOTAL // (N_REPLICA * SEQ_DEV))
    expert_ids_turns = jax.random.permutation(jax.random.fold_in(part_splits[9], 3), SEQUENCE_TOTAL // (N_REPLICA * SEQ_DEV))
    expert_ids = jax.vmap(lambda own, number: shared_out(jax.random.fold_in(part_splits[9], 2), own, number, N_REPLICA * SEQ_DEV, EXPERTS, TOPK, MOST, 2))(expert_ids_keys, expert_ids_turns).reshape((SEQUENCE_TOTAL, TOPK))
    route_weight = jnp.clip(jnp.exp(math.log(1.0) - 2.9957323 * jax.random.uniform(part_splits[10], (SEQUENCE_TOTAL, TOPK), jnp.float32) ** shard_levels(part_splits[10], (SEQUENCE_TOTAL, TOPK), ((0, 16),), -0.2, 0.2)), 0.05, 1.0)
    w_gate = normal_values(key_list[11], (EXPERTS, D, FF), D ** -0.5, 0.09375, ((0, 16), (2, 2)))
    w_up = normal_values(key_list[12], (EXPERTS, D, FF), D ** -0.5, 0.09375, ((0, 16), (2, 2)))
    w_down = normal_values(key_list[13], (EXPERTS, FF, D), (FF // 4) ** -0.5, 0.4375, ((0, 16), (1, 2)))
    return dict(queries=queries, token_keys=token_keys, token_values=token_values, stored_keys=stored_keys, stored_values=stored_values, kv_len=kv_len, residual=residual, out_weight=out_weight, norm_gain=norm_gain, expert_ids=expert_ids, route_weight=route_weight, w_gate=w_gate, w_up=w_up, w_down=w_down)


def attend(queries, token_keys, token_values, stored_keys, stored_values, kv_len):
    sequence_rows = queries.shape[0]
    query_group_width = QUERY_HEADS // KEY_VALUE_HEADS
    query_head_rows = queries.astype(jnp.float32).reshape(sequence_rows, KEY_VALUE_HEADS, query_group_width, HEAD_WIDTH)
    keys_from_cache = stored_keys.astype(jnp.float32).reshape(sequence_rows, CACHE_POSITIONS, KEY_VALUE_HEADS, HEAD_WIDTH)
    values_from_cache = stored_values.astype(jnp.float32).reshape(sequence_rows, CACHE_POSITIONS, KEY_VALUE_HEADS, HEAD_WIDTH)
    keys_latest = token_keys.astype(jnp.float32).reshape(sequence_rows, KEY_VALUE_HEADS, HEAD_WIDTH)
    values_latest = token_values.astype(jnp.float32).reshape(sequence_rows, KEY_VALUE_HEADS, HEAD_WIDTH)
    inv_root = 1.0 / math.sqrt(HEAD_WIDTH)
    cached_scores = jnp.einsum('bgqd,bpgd->bgqp', query_head_rows, keys_from_cache) * inv_root
    positions = jnp.arange(CACHE_POSITIONS, dtype=jnp.int32)
    visible = positions[None, :] < kv_len[:, None]
    cached_scores = jnp.where(visible[:, None, None, :], cached_scores, -jnp.inf)
    fresh_score = jnp.einsum('bgqd,bgd->bgq', query_head_rows, keys_latest) * inv_root
    highest = jnp.maximum(lax.optimization_barrier(jnp.max(cached_scores, axis=-1)), fresh_score)
    cached_exp = jnp.exp(cached_scores - highest[..., None])
    fresh_exp = jnp.exp(fresh_score - highest)
    totals = lax.optimization_barrier(jnp.sum(cached_exp, axis=-1)) + fresh_exp
    cached_prob = lax.optimization_barrier((cached_exp / totals[..., None]).astype(jnp.bfloat16)).astype(jnp.float32)
    fresh_prob = lax.optimization_barrier((fresh_exp / totals).astype(jnp.bfloat16)).astype(jnp.float32)
    mixed = jnp.einsum('bgqp,bpgd->bgqd', cached_prob, values_from_cache)
    mixed = mixed + fresh_prob[..., None] * values_latest[:, :, None, :]
    return mixed.reshape(sequence_rows, QUERY_HEADS * HEAD_WIDTH).astype(jnp.bfloat16)

def reference(queries, token_keys, token_values, stored_keys, stored_values, kv_len, residual, out_weight, norm_gain, expert_ids, route_weight, w_gate, w_up, w_down):
    attended = attend(queries, token_keys, token_values, stored_keys, stored_values, kv_len)
    hidden_state = residual.astype(jnp.float32) + jnp.dot(attended, out_weight, preferred_element_type=jnp.float32)
    mean_square = lax.optimization_barrier(jnp.mean(hidden_state * hidden_state, axis=-1, keepdims=True))
    normed = (hidden_state * lax.rsqrt(mean_square + 1e-06) * norm_gain.astype(jnp.float32)).astype(jnp.bfloat16)
    mixing = route_weight / lax.optimization_barrier(jnp.sum(route_weight, axis=1, keepdims=True))
    flat_ids = expert_ids.reshape(-1).astype(jnp.int32)
    row_total = flat_ids.shape[0]
    sorted_rows = jnp.argsort(flat_ids, stable=True).astype(jnp.int32)
    member = flat_ids[None, :] == jnp.arange(EXPERTS, dtype=jnp.int32)[:, None]
    counts = lax.optimization_barrier(jnp.sum(member.astype(jnp.int32), axis=1)).astype(jnp.int32)
    starts = (jnp.cumsum(counts) - counts).astype(jnp.int32)
    capacity = MOST * N_EXPERT

    def one_expert(expert):
        offsets = jnp.arange(capacity, dtype=jnp.int32)
        taken_rows = sorted_rows[jnp.clip(starts[expert] + offsets, 0, row_total - 1)]
        alive_slot = offsets < counts[expert]
        inputs = normed[taken_rows // TOPK]
        gate_act = jnp.dot(inputs, w_gate[expert], preferred_element_type=jnp.float32)
        up_act = jnp.dot(inputs, w_up[expert], preferred_element_type=jnp.float32)
        hidden_act = (jax.nn.silu(gate_act) * up_act).astype(jnp.bfloat16)
        output = jnp.dot(hidden_act, w_down[expert], preferred_element_type=jnp.float32)
        return (jnp.where(alive_slot[:, None], output, 0.0), taken_rows)
    outputs, taken_all = lax.map(one_expert, jnp.arange(EXPERTS, dtype=jnp.int32))
    weights = mixing.reshape(-1)[taken_all]
    moe_out = jnp.zeros((SEQUENCE_TOTAL, D), jnp.float32).at[(taken_all // TOPK).reshape(-1)].add((weights[..., None] * outputs).reshape(-1, D))
    return (hidden_state + moe_out).astype(jnp.bfloat16)
```

```python
import functools
import math

import jax
import jax.numpy as jnp
from jax import lax
from jax.experimental import pallas as pl
from jax.experimental.pallas import tpu as pltpu
from jax.sharding import PartitionSpec as P

HEAD_WIDTH = 128
TILE = 16
MESH = pl.DeviceIdType.MESH
F32 = jnp.float32
BF16 = jnp.bfloat16


def permutation(size, source):
    a = lax.broadcasted_iota(jnp.int32, (size, 8 * TILE), 0)
    b = lax.broadcasted_iota(jnp.int32, (size, 8 * TILE), 1)
    return jnp.where(b == source(a), 1.0, 0.0).astype(BF16)


def heads_out(hpc, S):
    return permutation(
        8 * hpc * S,
        lambda a: ((a // S) % 8) * TILE + (a % S) * hpc + a // (8 * S),
    )


def parts_out(Q, cap):
    return permutation(
        8 * Q * cap,
        lambda a: ((a // cap) % 8) * TILE + (a // (8 * cap)) * cap + a % cap,
    )


def parts_in(Q, cap):
    return permutation(
        8 * Q * cap,
        lambda a: ((a % TILE) // cap) * 8 * cap + (a // TILE) * cap + a % cap,
    )


def dot(a, b):
    return jnp.dot(a, b, preferred_element_type=F32)


def kernel(
    E, I, cap,
    q_hbm, tk_hbm, tv_hbm, kv_hbm, res_hbm, gain_hbm, ids_hbm, rw_hbm,
    k_hbm, v_hbm, ow_hbm, wg_hbm, wu_hbm, wd_hbm,
    out_hbm,
    q_ref, tk_ref, tv_ref, kv_ref, res_ref, gain_ref, ids_ref, rw_ref,
    kb, vb, owo, ow, wg, wu, wd,
    qs, tks, tvs, attf, att, ratt, asm,
    ya, rsa, yb, rsb, zb, rsc,
    resb, resp, hs, tts, whi, wlo,
    xb, xr, xs, gus, gur, hid, zs, zr, ub, up_, outb,
    isem, ksem, wsem, outsem, psend, precv,
    s1, r1, sa, ra, sb, rb, sc, rc, sx, rx, sz, rz,
):
    N = 2 * E
    O = E // I
    bits = E.bit_length() - 1
    e_me = lax.axis_index("expert")
    c = lax.axis_index("replica")
    rank = e_me * 2 + c
    S = q_ref.shape[0]
    T = 2 * S
    heads = q_ref.shape[1] // HEAD_WIDTH
    G = tk_ref.shape[1] // HEAD_WIDTH
    width = heads // G
    L = k_hbm.shape[1]
    D = res_ref.shape[1]
    half = D // 2
    hpc = heads // E
    Q = TILE // cap
    wide = half // 2
    piece = wide // Q
    FH = wg_hbm.shape[2]
    orow = ow_hbm.shape[0]
    drow = wd_hbm.shape[1]
    mine = pl.ds(pl.multiple_of(c * half, half), half)
    other = pl.ds(pl.multiple_of((1 - c) * half, half), half)
    omine = pl.ds(pl.multiple_of(c * orow, orow), orow)
    dmine = pl.ds(pl.multiple_of(c * drow, drow), drow)
    fmine = pl.ds(pl.multiple_of(c * FH, FH), FH)

    place = []
    for k in range(bits):
        bit = lax.rem(lax.div(e_me, 1 << k), 2)
        place.append((bit * (1 << k), (1 - bit) * (1 << k)))

    def expert_at(mask):
        return functools.reduce(lambda a, b: a + b, [place[k][(mask >> k) & 1] for k in range(bits)])

    peer = [expert_at(m) for m in range(E)]
    side = [c, 1 - c]
    order = {m: (m % I) * O + m // I for m in range(E)}

    small = [
        pltpu.make_async_copy(src, dst, isem.at[k])
        for k, (src, dst) in enumerate((
            (q_hbm, q_ref), (tk_hbm, tk_ref), (tv_hbm, tv_ref), (kv_hbm, kv_ref),
            (res_hbm, res_ref), (gain_hbm, gain_ref), (ids_hbm, ids_ref), (rw_hbm, rw_ref),
        ))
    ]
    kcopies = [
        pltpu.make_async_copy(k_hbm.at[b], kb.at[pl.ds(b * L, L)], ksem.at[b]) for b in range(S)
    ]
    vcopies = [
        pltpu.make_async_copy(v_hbm.at[b], vb.at[pl.ds(b * L, L)], ksem.at[S + b]) for b in range(S)
    ]
    wcopies = [
        pltpu.make_async_copy(ow_hbm.at[:, other], owo, wsem.at[0]),
        pltpu.make_async_copy(ow_hbm.at[:, mine], ow.at[omine], wsem.at[1]),
        pltpu.make_async_copy(wg_hbm.at[0, mine], wg.at[:, fmine], wsem.at[2]),
        pltpu.make_async_copy(wu_hbm.at[0, mine], wu.at[:, fmine], wsem.at[3]),
        pltpu.make_async_copy(wd_hbm.at[0, :, mine], wd.at[dmine], wsem.at[4]),
    ]
    for cp in small[:4] + kcopies + vcopies:
        cp.start()
    barrier = pltpu.get_barrier_semaphore()
    for m in range(E - 1, -1, -1):
        for k in (0, 1):
            if m or k:
                pl.semaphore_signal(
                    barrier, inc=1,
                    device_id={"expert": peer[m], "replica": side[k]}, device_id_type=MESH,
                )
    for cp in small[4:]:
        cp.start()

    for cp in small[:4]:
        cp.wait()
    qf = q_ref[...].astype(F32)
    for h in range(heads):
        qs[pl.ds(S * h, S), :] = qf[:, h * HEAD_WIDTH:(h + 1) * HEAD_WIDTH]
    tks[0:S, :] = tk_ref[...].astype(F32)
    tvs[0:S, :] = tv_ref[...].astype(F32)
    if hpc * S < TILE:
        attf[...] = jnp.zeros_like(attf)
    inv_root = 1.0 / math.sqrt(HEAD_WIDTH)
    group = lax.broadcasted_iota(jnp.int32, (heads, HEAD_WIDTH), 0) // width
    col = lax.broadcasted_iota(jnp.int32, (heads, L), 1)

    def by_head(ref, b):
        return jnp.concatenate([
            jnp.broadcast_to(ref[b:b + 1, g * HEAD_WIDTH:(g + 1) * HEAD_WIDTH], (width, HEAD_WIDTH))
            for g in range(G)
        ], axis=0)

    rows_q = []
    fresh = []
    for b in range(S):
        qb = qs[pl.ds(b, heads, stride=S), :]
        rows_q.append(jnp.concatenate(
            [jnp.where(group == g, qb, 0.0).astype(BF16) for g in range(G)], axis=1
        ))
        fresh.append(jnp.sum(qb * by_head(tks, b), axis=1, keepdims=True) * inv_root)
    for cp in kcopies:
        cp.wait()
    probs = []
    fprobs = []
    for b in range(S):
        score = lax.dot_general(
            rows_q[b], kb[b * L:(b + 1) * L, :], (((1,), (1,)), ((), ())),
            preferred_element_type=F32,
        ) * inv_root
        score = jnp.where(col < kv_ref[b], score, -jnp.inf)
        top = jnp.maximum(jnp.max(score, axis=1, keepdims=True), fresh[b])
        ex = jnp.exp(score - top)
        fex = jnp.exp(fresh[b] - top)
        inv = 1.0 / (jnp.sum(ex, axis=1, keepdims=True) + fex)
        probs.append((ex * inv).astype(BF16))
        fprobs.append((fex * inv).astype(BF16).astype(F32))
    for cp in vcopies:
        cp.wait()
    for cp in wcopies:
        cp.start()
    for b in range(S):
        o = dot(probs[b], vb[b * L:(b + 1) * L, :])
        o = jnp.concatenate([
            o[g * width:(g + 1) * width, g * HEAD_WIDTH:(g + 1) * HEAD_WIDTH] for g in range(G)
        ], axis=0)
        o = o + fprobs[b] * by_head(tvs, b)
        for j in range(E):
            attf[j * TILE + b * hpc:j * TILE + (b + 1) * hpc, :] = o[j * hpc:(j + 1) * hpc]
    att[...] = attf[...].astype(BF16)

    pl.semaphore_wait(barrier, N - 1)

    def rows_at(start, count):
        return pl.ds(pl.multiple_of(start * TILE, TILE), count * TILE)

    def att_copy(m, k):
        return pltpu.make_async_remote_copy(
            src_ref=att.at[rows_at(peer[m], 1)], dst_ref=ratt.at[rows_at(2 * order[m] + c, 1)],
            send_sem=s1.at[2 * m + k], recv_sem=r1.at[2 * m + k],
            device_id={"expert": peer[m], "replica": side[k]}, device_id_type=MESH,
        )

    def to_peer(src, dst, send, recv, m):
        return pltpu.make_async_remote_copy(
            src_ref=src, dst_ref=dst, send_sem=send, recv_sem=recv,
            device_id={"expert": peer[m], "replica": c}, device_id_type=MESH,
        )

    def beside(src, dst, k):
        return pltpu.make_async_remote_copy(
            src_ref=src, dst_ref=dst, send_sem=psend.at[k], recv_sem=precv.at[k],
            device_id={"expert": e_me, "replica": 1 - c}, device_id_type=MESH,
        )

    far_first = range(E - 1, 0, -1)
    att_x = [att_copy(m, k) for m in far_first for k in (0, 1)] + [att_copy(0, 1)]
    for cp in att_x:
        cp.start()
    wcopies[0].wait()
    ow_x = beside(owo, ow.at[omine], 0)
    ow_x.start()
    for cp in small[4:]:
        cp.wait()
    ratt[rows_at(c, 1)] = att[rows_at(e_me, 1)]
    for rep in range(8 // S):
        resb[pl.ds(rep * S, S), :] = res_ref[...].astype(F32)
    res_x = beside(resb.at[:, other], resp, 1)
    res_x.start()

    lanes_all = E * TILE
    lane = lax.broadcasted_iota(jnp.int32, (T, lanes_all), 1)
    tok = lax.broadcasted_iota(jnp.int32, (T, lanes_all), 0)
    lm = lane // TILE
    le = jnp.zeros((T, lanes_all), jnp.int32)
    for k in range(bits):
        flip = (lm // (1 << k)) % 2
        le = le + jnp.where(flip == 1, place[k][1], place[k][0])
    lq = (lane // cap) % Q
    ls = lane % cap
    ids = ids_ref[...]
    rw = rw_ref[...]
    mix = rw / jnp.sum(rw, axis=1, keepdims=True)
    named = jnp.zeros((T, lanes_all), F32)
    weight = jnp.zeros((T, lanes_all), F32)
    for k in range(ids.shape[1]):
        hit = ids[:, k:k + 1] == le
        named = named + jnp.where(hit, 1.0, 0.0)
        weight = weight + jnp.where(hit, mix[:, k:k + 1], 0.0)
    before = jnp.zeros((T, lanes_all), F32)
    for t in range(T - 1):
        before = before + jnp.where(tok > t, named[t:t + 1, :], 0.0)
    chosen = jnp.where(before == ls.astype(F32), named, 0.0)
    weight = weight * chosen
    high = weight.astype(BF16).astype(F32)
    low = weight - high
    for p in range(Q):
        here = lq == p
        tts[p * T:(p + 1) * T, :] = jnp.where(here, chosen, 0.0)
        whi[p * T:(p + 1) * T, :] = jnp.where(here, high, 0.0)
        wlo[p * T:(p + 1) * T, :] = jnp.where(here, low, 0.0)

    wcopies[1].wait()
    ow_x.wait()
    for cp in att_x:
        cp.wait_recv()

    pa = heads_out(hpc, S)
    for grp in range(N // 8):
        blk = dot(pa, ratt[grp * 8 * TILE:(grp + 1) * 8 * TILE, :]).astype(BF16)
        for h in range(hpc):
            asm[grp * 8 * S:(grp + 1) * 8 * S, h * HEAD_WIDTH:(h + 1) * HEAD_WIDTH] = (
                blk[h * 8 * S:(h + 1) * 8 * S]
            )
    lanes = wide // 2

    def project(chunk):
        y = [
            dot(asm[...], ow[:, chunk * wide + j * lanes:chunk * wide + (j + 1) * lanes])
            for j in (0, 1)
        ]
        both = jnp.concatenate([v.reshape(E, T, lanes) for v in y], axis=1)
        return both.reshape(E * TILE, lanes).astype(BF16)

    inner = range(1, I)
    outer = range(1, O)
    yb[...] = project(1)
    b_x = [
        to_peer(yb.at[rows_at(p * O, O)], rsb.at[p], sb.at[p], rb.at[p], p) for p in inner
    ]
    for cp in b_x:
        cp.start()
    ya[...] = project(0)
    a_x = [
        to_peer(
            ya.at[rows_at(order[m], 1)], rsa.at[rows_at(order[m], 1)], sa.at[m], ra.at[m], m
        )
        for m in far_first
    ]
    for cp in a_x:
        cp.start()
    wg_x = beside(wg_hbm.at[0, other], wg.at[:, fmine], 2)
    wu_x = beside(wu_hbm.at[0, other], wu.at[:, fmine], 3)
    wd_x = beside(wd_hbm.at[0, :, other], wd.at[dmine], 4)
    for cp in (wg_x, wu_x, wd_x):
        cp.start()

    for cp in b_x:
        cp.wait_recv()
    relay = yb[0:O * TILE, :].astype(F32)
    for p in inner:
        relay = relay + rsb[p].astype(F32)
    zb[...] = relay.astype(BF16)
    c_x = [
        to_peer(zb.at[rows_at(o, 1)], rsc.at[rows_at(o, 1)], sc.at[o], rc.at[o], o * I)
        for o in reversed(outer)
    ]
    for cp in c_x:
        cp.start()
    kept = relay[0:TILE]

    res_x.wait()
    for cp in att_x:
        cp.wait_send()
    trow = lax.broadcasted_iota(jnp.int32, (T, half), 0)
    base = jnp.where(trow // S == c, resb[:, mine], resp[...])
    table = tts[...].astype(BF16)

    def dispatch(chunk, total):
        hidden = base[:, chunk * wide:(chunk + 1) * wide] + jnp.concatenate(
            [total[:T], total[T:]], axis=1
        )
        hs[:, chunk * wide:(chunk + 1) * wide] = hidden
        stacked = jnp.concatenate(
            [hidden[:, p * piece:(p + 1) * piece] for p in range(Q)], axis=0
        ).astype(BF16)
        picked = lax.dot_general(
            table, stacked, (((0,), (0,)), ((), ())), preferred_element_type=F32
        ).astype(BF16)
        xb[chunk] = picked
        copies = [
            to_peer(
                xb.at[chunk, rows_at(m, 1)], xr.at[chunk, rows_at(m, 1)],
                sx.at[chunk, m], rx.at[chunk, m], m,
            )
            for m in far_first
        ]
        for cp in copies:
            cp.start()
        xr[chunk, 0:TILE] = picked[0:TILE]
        return copies

    for cp in a_x:
        cp.wait_recv()
    total = ya[0:TILE, :].astype(F32)
    for m in range(1, E):
        total = total + rsa[m * TILE:(m + 1) * TILE, :].astype(F32)
    x_x = [dispatch(0, total)]
    for cp in c_x:
        cp.wait_recv()
    total = kept
    for o in outer:
        total = total + rsc[o * TILE:(o + 1) * TILE, :].astype(F32)
    x_x.append(dispatch(1, total))

    for cp in wcopies[2:]:
        cp.wait()
    wg_x.wait()
    wu_x.wait()
    wd_x.wait()
    for cp in a_x + b_x + c_x:
        cp.wait_send()
    px = parts_out(Q, cap)
    gc = 8 * cap
    rows = E * cap
    gain = gain_ref[mine].astype(F32).reshape(1, half)
    square = jnp.zeros((rows, 1), F32)
    F = 2 * FH
    for k in range(2):
        for cp in x_x[k]:
            cp.wait_recv()
        blk = [
            dot(px, xr[k, grp * 8 * TILE:(grp + 1) * 8 * TILE, :]) for grp in range(E // 8)
        ]
        for p in range(Q):
            part = jnp.concatenate([v[p * gc:(p + 1) * gc] for v in blk], axis=0)
            square = square + jnp.sum(part * part, axis=1, keepdims=True)
            cols = slice(k * wide + p * piece, k * wide + (p + 1) * piece)
            xs[:, cols] = (part * gain[:, cols]).astype(BF16)
        feats = slice(k * wide, (k + 1) * wide)
        if k == 0:
            gus[:, 128:128 + F] = dot(xs[:, feats], wg[feats, :])
            gus[:, 128 + F:128 + 2 * F] = dot(xs[:, feats], wu[feats, :])
        else:
            gus[:, 0:128] = jnp.broadcast_to(square, (rows, 128))
            gus[:, 128:128 + F] += dot(xs[:, feats], wg[feats, :])
            first = pl.ds(0, 128 + F)
            g_x = beside(gus.at[:, first], gur.at[:, first], 5)
            g_x.start()
            gus[:, 128 + F:128 + 2 * F] += dot(xs[:, feats], wu[feats, :])
            second = pl.ds(128 + F, F)
            u_x = beside(gus.at[:, second], gur.at[:, second], 6)
            u_x.start()
    g_x.wait()
    scale = lax.rsqrt((gus[:, 0:1] + gur[:, 0:1]) / D + 1e-06)
    gate = (gus[:, 128:128 + F] + gur[:, 128:128 + F]) * scale
    gate = gate / (1.0 + jnp.exp(-gate))
    u_x.wait()
    up = (gus[:, 128 + F:128 + 2 * F] + gur[:, 128 + F:128 + 2 * F]) * scale
    hid[...] = (gate * up).astype(BF16)

    pb = parts_in(Q, cap)
    z_x = []
    for k in range(2):
        o = dot(hid[...], wd[:, k * wide:(k + 1) * wide]).astype(BF16)
        for grp in range(E // 8):
            blk = jnp.concatenate([
                o[grp * gc:(grp + 1) * gc, p * piece:(p + 1) * piece] for p in range(Q)
            ], axis=0)
            zs[k, grp * 8 * TILE:(grp + 1) * 8 * TILE, :] = dot(pb, blk).astype(BF16)
        copies = [
            to_peer(
                zs.at[k, rows_at(m, 1)], zr.at[k, rows_at(m, 1)], sz.at[k, m], rz.at[k, m], m
            )
            for m in far_first
        ]
        for cp in copies:
            cp.start()
        zr[k, 0:TILE] = zs[k, 0:TILE]
        z_x.append(copies)

    for k in range(2):
        for cp in x_x[k]:
            cp.wait_send()
    wh = whi[...].astype(BF16)
    wl = wlo[...].astype(BF16)
    own = c == 0
    f_x = []
    for k in range(2):
        for cp in z_x[k]:
            cp.wait_recv()
        part = dot(wh, zr[k]) + dot(wl, zr[k])
        cols = slice(k * wide, (k + 1) * wide)
        updated = hs[:, cols] + jnp.concatenate(
            [part[p * T:(p + 1) * T] for p in range(Q)], axis=1
        )
        ub[:, cols] = updated
        f_x.append(beside(ub.at[:, pl.ds(k * wide, wide)], up_.at[:, pl.ds(k * wide, wide)], 7 + k))
        f_x[k].start()
        at = pl.ds(pl.multiple_of(c * half + k * wide, wide), wide)
        outb[:, at] = jnp.where(own, updated[:S], updated[S:]).astype(BF16)
    outs = [pltpu.make_async_copy(outb.at[:, mine], out_hbm.at[:, mine], outsem.at[0])]
    outs[0].start()
    for k in range(2):
        for cp in z_x[k]:
            cp.wait_send()
    for cp in f_x:
        cp.wait()
    got = up_[...]
    outb[:, other] = jnp.where(own, got[:S], got[S:]).astype(BF16)
    outs.append(pltpu.make_async_copy(outb.at[:, other], out_hbm.at[:, other], outsem.at[1]))
    outs[1].start()
    for cp in outs:
        cp.wait()


def on_device(
    queries, token_keys, token_values, stored_keys, stored_values, kv_len, residual, out_weight,
    norm_gain, expert_ids, route_weight, w_gate, w_up, w_down,
):
    E = lax.axis_size("expert")
    N = 2 * E
    I = 1 << ((E.bit_length() - 1) // 2)
    O = E // I
    S, features = queries.shape
    T = 2 * S
    L = stored_keys.shape[1]
    KW = token_keys.shape[1]
    D = residual.shape[1]
    half = D // 2
    wide = half // 2
    topk = expert_ids.shape[1]
    FH = w_gate.shape[2]
    cap = max(2, -(-(T * topk) // E))
    Q = TILE // cap
    piece = wide // Q
    orow = out_weight.shape[0]
    hbm = pl.BlockSpec(memory_space=pltpu.HBM)
    V = pltpu.VMEM
    dma = pltpu.SemaphoreType.DMA
    wout = 128 + 4 * FH
    scratch = [
        V((S, features), BF16), V((S, KW), BF16), V((S, KW), BF16), pltpu.SMEM((S,), jnp.int32),
        V((S, D), BF16), V((D,), BF16), V(expert_ids.shape, jnp.int32), V(route_weight.shape, F32),
        V((S * L, KW), BF16), V((S * L, KW), BF16),
        V((orow, half), BF16), V((2 * orow, half), BF16),
        V((half, 2 * FH), BF16), V((half, 2 * FH), BF16), V((2 * FH, half), BF16),
        V((S * features // HEAD_WIDTH, HEAD_WIDTH), F32), V((8, KW), F32), V((8, KW), F32),
        V((E * TILE, HEAD_WIDTH), F32), V((E * TILE, HEAD_WIDTH), BF16),
        V((N * TILE, HEAD_WIDTH), BF16), V((N * S, 2 * orow), BF16),
        V((E * TILE, wide // 2), BF16), V((E * TILE, wide // 2), BF16),
        V((E * TILE, wide // 2), BF16), V((I, O * TILE, wide // 2), BF16),
        V((O * TILE, wide // 2), BF16), V((O * TILE, wide // 2), BF16),
        V((T, D), F32), V((T, half), F32), V((T, half), F32),
        V((Q * T, E * TILE), F32), V((Q * T, E * TILE), F32), V((Q * T, E * TILE), F32),
        V((2, E * TILE, piece), BF16), V((2, E * TILE, piece), BF16), V((E * cap, half), BF16),
        V((E * cap, wout), F32), V((E * cap, wout), F32), V((E * cap, 2 * FH), BF16),
        V((2, E * TILE, piece), BF16), V((2, E * TILE, piece), BF16),
        V((T, half), F32), V((T, half), F32), V((S, D), BF16),
        dma((8,)), dma((2 * S,)), dma((5,)), dma((2,)), dma((9,)), dma((9,)),
        dma((N,)), dma((N,)), dma((E,)), dma((E,)), dma((I,)), dma((I,)), dma((O,)), dma((O,)),
        dma((2, E)), dma((2, E)), dma((2, E)), dma((2, E)),
    ]
    return pl.pallas_call(
        functools.partial(kernel, E, I, cap),
        out_shape=jax.ShapeDtypeStruct((S, D), BF16),
        in_specs=[hbm] * 14,
        out_specs=hbm,
        scratch_shapes=scratch,
        compiler_params=pltpu.CompilerParams(
            collective_id=0, has_side_effects=True, vmem_limit_bytes=67043328
        ),
    )(
        queries, token_keys, token_values, kv_len, residual, norm_gain, expert_ids,
        route_weight, stored_keys, stored_values, out_weight, w_gate, w_up, w_down,
    )


def solution(mesh):
    rows = P(("groups", "expert", "replica"), None)
    cube = P(("groups", "expert", "replica"), None, None)
    in_specs = (
        rows, rows, rows, cube, cube, P(("groups", "expert", "replica")), rows,
        P(("expert", "replica"), None), P(), P(("groups", "expert"), None),
        P(("groups", "expert"), None), P("expert", None, "replica"),
        P("expert", None, "replica"), P("expert", "replica", None),
    )
    return jax.shard_map(
        on_device, mesh=mesh, in_specs=in_specs, out_specs=rows, check_vma=False
    )
```

```python
import functools
import math

import jax
import jax.numpy as jnp
from jax import lax
from jax.experimental import pallas as pl
from jax.experimental.pallas import tpu as pltpu
from jax.sharding import PartitionSpec as P

HEAD_WIDTH = 128
TILE = 16
MESH = pl.DeviceIdType.MESH
F32 = jnp.float32
BF16 = jnp.bfloat16


def permutation(size, source):
    a = lax.broadcasted_iota(jnp.int32, (size, 8 * TILE), 0)
    b = lax.broadcasted_iota(jnp.int32, (size, 8 * TILE), 1)
    return jnp.where(b == source(a), 1.0, 0.0).astype(BF16)


def heads_out(hpc, S):
    return permutation(
        8 * hpc * S,
        lambda a: ((a // S) % 8) * TILE + (a % S) * hpc + a // (8 * S),
    )


def parts_out(Q, cap):
    return permutation(
        8 * Q * cap,
        lambda a: ((a // cap) % 8) * TILE + (a // (8 * cap)) * cap + a % cap,
    )


def parts_in(Q, cap):
    return permutation(
        8 * Q * cap,
        lambda a: ((a % TILE) // cap) * 8 * cap + (a // TILE) * cap + a % cap,
    )


def dot(a, b):
    return jnp.dot(a, b, preferred_element_type=F32)


def kernel(
    E, I, cap,
    q_hbm, tk_hbm, tv_hbm, kv_hbm, res_hbm, gain_hbm, ids_hbm, rw_hbm,
    k_hbm, v_hbm, ow_hbm, wg_hbm, wu_hbm, wd_hbm,
    out_ref,
    q_ref, tk_ref, tv_ref, kv_ref, res_ref, gain_ref, ids_ref, rw_ref,
    kb, vb, owo, ow, wg, wu, wd,
    qs, tks, tvs, attf, att, ratt, asm,
    ya, rsa, yb, rsb, zb, rsc,
    resb, resp, hs, tts, whi, wlo,
    xb, xr, xs, gus, gur, hid, zs, zr, ub, up_,
    isem, ksem, wsem, psend, precv,
    s1, r1, sa, ra, sb, rb, sc, rc, sx, rx, sz, rz,
):
    N = 2 * E
    O = E // I
    bits = E.bit_length() - 1
    e_me = lax.axis_index("expert")
    c = lax.axis_index("replica")
    rank = e_me * 2 + c
    S = q_ref.shape[0]
    T = 2 * S
    heads = q_ref.shape[1] // HEAD_WIDTH
    G = tk_ref.shape[1] // HEAD_WIDTH
    width = heads // G
    L = k_hbm.shape[1]
    D = res_ref.shape[1]
    half = D // 2
    hpc = heads // E
    Q = TILE // cap
    wide = half // 2
    piece = HEAD_WIDTH
    step = Q * piece
    C = half // step
    FH = wg_hbm.shape[2]
    orow = ow_hbm.shape[0]
    drow = wd_hbm.shape[1]
    mine = pl.ds(pl.multiple_of(c * half, half), half)
    other = pl.ds(pl.multiple_of((1 - c) * half, half), half)
    omine = pl.ds(pl.multiple_of(c * orow, orow), orow)
    dmine = pl.ds(pl.multiple_of(c * drow, drow), drow)
    fmine = pl.ds(pl.multiple_of(c * FH, FH), FH)

    place = []
    for k in range(bits):
        bit = lax.rem(lax.div(e_me, 1 << k), 2)
        place.append((bit * (1 << k), (1 - bit) * (1 << k)))

    def expert_at(mask):
        return functools.reduce(lambda a, b: a + b, [place[k][(mask >> k) & 1] for k in range(bits)])

    peer = [expert_at(m) for m in range(E)]
    side = [c, 1 - c]
    order = {m: (m % I) * O + m // I for m in range(E)}

    small = [
        pltpu.make_async_copy(src, dst, isem.at[k])
        for k, (src, dst) in enumerate((
            (q_hbm, q_ref), (tk_hbm, tk_ref), (tv_hbm, tv_ref), (kv_hbm, kv_ref),
            (res_hbm, res_ref), (gain_hbm, gain_ref), (ids_hbm, ids_ref), (rw_hbm, rw_ref),
        ))
    ]
    k_copy = pltpu.make_async_copy(k_hbm, kb, ksem.at[0])
    v_copy = pltpu.make_async_copy(v_hbm, vb, ksem.at[1])
    wcopies = [
        pltpu.make_async_copy(ow_hbm.at[:, other], owo, wsem.at[0]),
        pltpu.make_async_copy(ow_hbm.at[:, mine], ow.at[omine], wsem.at[1]),
        pltpu.make_async_copy(wg_hbm.at[0, mine], wg.at[:, fmine], wsem.at[2]),
        pltpu.make_async_copy(wu_hbm.at[0, mine], wu.at[:, fmine], wsem.at[3]),
        pltpu.make_async_copy(wd_hbm.at[0, :, mine], wd.at[dmine], wsem.at[4]),
    ]
    for cp in small[:4] + [k_copy, v_copy]:
        cp.start()
    barrier = pltpu.get_barrier_semaphore()
    for m in range(E - 1, -1, -1):
        for k in (0, 1):
            if m or k:
                pl.semaphore_signal(
                    barrier, inc=1,
                    device_id={"expert": peer[m], "replica": side[k]}, device_id_type=MESH,
                )
    for cp in small[4:]:
        cp.start()

    for cp in small[:4]:
        cp.wait()
    qf = q_ref[...].astype(F32)
    for h in range(heads):
        qs[pl.ds(S * h, S), :] = qf[:, h * HEAD_WIDTH:(h + 1) * HEAD_WIDTH]
    tks[0:S, :] = tk_ref[...].astype(F32)
    tvs[0:S, :] = tv_ref[...].astype(F32)
    if hpc * S < TILE:
        attf[...] = jnp.zeros_like(attf)
    inv_root = 1.0 / math.sqrt(HEAD_WIDTH)
    group = lax.broadcasted_iota(jnp.int32, (heads, HEAD_WIDTH), 0) // width
    col = lax.broadcasted_iota(jnp.int32, (heads, L), 1)

    def by_head(ref, b):
        return jnp.concatenate([
            jnp.broadcast_to(ref[b:b + 1, g * HEAD_WIDTH:(g + 1) * HEAD_WIDTH], (width, HEAD_WIDTH))
            for g in range(G)
        ], axis=0)

    rows_q = []
    fresh = []
    for b in range(S):
        qb = qs[pl.ds(b, heads, stride=S), :]
        rows_q.append(jnp.concatenate(
            [jnp.where(group == g, qb, 0.0).astype(BF16) for g in range(G)], axis=1
        ))
        fresh.append(jnp.sum(qb * by_head(tks, b), axis=1, keepdims=True) * inv_root)
    k_copy.wait()
    probs = []
    fprobs = []
    for b in range(S):
        score = lax.dot_general(
            rows_q[b], kb[b], (((1,), (1,)), ((), ())),
            preferred_element_type=F32,
        ) * inv_root
        score = jnp.where(col < kv_ref[b], score, -jnp.inf)
        top = jnp.maximum(jnp.max(score, axis=1, keepdims=True), fresh[b])
        ex = jnp.exp(score - top)
        fex = jnp.exp(fresh[b] - top)
        inv = 1.0 / (jnp.sum(ex, axis=1, keepdims=True) + fex)
        probs.append((ex * inv).astype(BF16))
        fprobs.append((fex * inv).astype(BF16).astype(F32))
    v_copy.wait()
    for cp in wcopies:
        cp.start()
    for b in range(S):
        o = dot(probs[b], vb[b])
        o = jnp.concatenate([
            o[g * width:(g + 1) * width, g * HEAD_WIDTH:(g + 1) * HEAD_WIDTH] for g in range(G)
        ], axis=0)
        o = o + fprobs[b] * by_head(tvs, b)
        for j in range(E):
            attf[j * TILE + b * hpc:j * TILE + (b + 1) * hpc, :] = o[j * hpc:(j + 1) * hpc]
    att[...] = attf[...].astype(BF16)

    pl.semaphore_wait(barrier, N - 1)

    def rows_at(start, count):
        return pl.ds(pl.multiple_of(start * TILE, TILE), count * TILE)

    def att_copy(m, k):
        return pltpu.make_async_remote_copy(
            src_ref=att.at[rows_at(peer[m], 1)], dst_ref=ratt.at[rows_at(2 * order[m] + c, 1)],
            send_sem=s1.at[0], recv_sem=r1.at[0],
            device_id={"expert": peer[m], "replica": side[k]}, device_id_type=MESH,
        )

    def to_peer(src, dst, send, recv, m):
        return pltpu.make_async_remote_copy(
            src_ref=src, dst_ref=dst, send_sem=send, recv_sem=recv,
            device_id={"expert": peer[m], "replica": c}, device_id_type=MESH,
        )

    def beside(src, dst, k):
        return pltpu.make_async_remote_copy(
            src_ref=src, dst_ref=dst, send_sem=psend.at[k], recv_sem=precv.at[k],
            device_id={"expert": e_me, "replica": 1 - c}, device_id_type=MESH,
        )

    def whole(ref, send, recv):
        return to_peer(ref, ref, send, recv, E - 1)

    far_first = range(E - 1, 0, -1)
    att_x = [att_copy(m, k) for m in far_first for k in (0, 1)] + [att_copy(0, 1)]
    for cp in att_x:
        cp.start()
    att_all = whole(ratt.at[rows_at(0, N - 1)], s1.at[0], r1.at[0])
    wcopies[0].wait()
    ow_x = beside(owo, ow.at[omine], 0)
    ow_x.start()
    for cp in small[4:]:
        cp.wait()
    ratt[rows_at(c, 1)] = att[rows_at(e_me, 1)]
    for rep in range(8 // S):
        resb[pl.ds(rep * S, S), :] = res_ref[...].astype(F32)
    res_x = beside(resb.at[:, other], resp, 1)
    res_x.start()

    lanes_all = E * TILE
    lane = lax.broadcasted_iota(jnp.int32, (T, lanes_all), 1)
    tok = lax.broadcasted_iota(jnp.int32, (T, lanes_all), 0)
    lm = lane // TILE
    le = jnp.zeros((T, lanes_all), jnp.int32)
    for k in range(bits):
        flip = (lm // (1 << k)) % 2
        le = le + jnp.where(flip == 1, place[k][1], place[k][0])
    lq = (lane // cap) % Q
    ls = lane % cap
    ids = ids_ref[...]
    rw = rw_ref[...]
    mix = rw / jnp.sum(rw, axis=1, keepdims=True)
    named = jnp.zeros((T, lanes_all), F32)
    weight = jnp.zeros((T, lanes_all), F32)
    for k in range(ids.shape[1]):
        hit = ids[:, k:k + 1] == le
        named = named + jnp.where(hit, 1.0, 0.0)
        weight = weight + jnp.where(hit, mix[:, k:k + 1], 0.0)
    before = jnp.zeros((T, lanes_all), F32)
    for t in range(T - 1):
        before = before + jnp.where(tok > t, named[t:t + 1, :], 0.0)
    chosen = jnp.where(before == ls.astype(F32), named, 0.0)
    weight = weight * chosen
    high = weight.astype(BF16).astype(F32)
    low = weight - high
    for p in range(Q):
        here = lq == p
        tts[p * T:(p + 1) * T, :] = jnp.where(here, chosen, 0.0)
        whi[p * T:(p + 1) * T, :] = jnp.where(here, high, 0.0)
        wlo[p * T:(p + 1) * T, :] = jnp.where(here, low, 0.0)

    wcopies[1].wait()
    ow_x.wait()
    att_all.wait_recv()

    pa = heads_out(hpc, S)
    for grp in range(N // 8):
        blk = dot(pa, ratt[grp * 8 * TILE:(grp + 1) * 8 * TILE, :]).astype(BF16)
        for h in range(hpc):
            asm[grp * 8 * S:(grp + 1) * 8 * S, h * HEAD_WIDTH:(h + 1) * HEAD_WIDTH] = (
                blk[h * 8 * S:(h + 1) * 8 * S]
            )
    lanes = wide // 2

    def project(chunk):
        y = [
            dot(asm[...], ow[:, chunk * wide + j * lanes:chunk * wide + (j + 1) * lanes])
            for j in (0, 1)
        ]
        both = jnp.concatenate([v.reshape(E, T, lanes) for v in y], axis=1)
        return both.reshape(E * TILE, lanes).astype(BF16)

    inner = range(1, I)
    outer = range(1, O)
    yb[...] = project(1)
    b_x = [
        to_peer(yb.at[rows_at(p * O, O)], rsb.at[p], sb.at[0], rb.at[0], p) for p in inner
    ]
    for cp in b_x:
        cp.start()
    ya[...] = project(0)
    a_x = [
        to_peer(
            ya.at[rows_at(order[m], 1)], rsa.at[rows_at(order[m], 1)], sa.at[0], ra.at[0], m
        )
        for m in far_first
    ]
    for cp in a_x:
        cp.start()
    wg_x = beside(wg_hbm.at[0, other], wg.at[:, fmine], 2)
    wu_x = beside(wu_hbm.at[0, other], wu.at[:, fmine], 3)
    wd_x = beside(wd_hbm.at[0, :, other], wd.at[dmine], 4)
    for cp in (wg_x, wu_x, wd_x):
        cp.start()

    b_all = whole(rsb.at[pl.ds(1, I - 1)], sb.at[0], rb.at[0])
    b_all.wait_recv()
    relay = yb[0:O * TILE, :].astype(F32)
    for p in inner:
        relay = relay + rsb[p].astype(F32)
    zb[...] = relay.astype(BF16)
    c_x = [
        to_peer(zb.at[rows_at(o, 1)], rsc.at[rows_at(o, 1)], sc.at[0], rc.at[0], o * I)
        for o in reversed(outer)
    ]
    for cp in c_x:
        cp.start()
    kept = relay[0:TILE]

    res_x.wait()
    att_all.wait_send()
    trow = lax.broadcasted_iota(jnp.int32, (T, half), 0)
    base = jnp.where(trow // S == c, resb[:, mine], resp[...])
    table = tts[...].astype(BF16)

    x_x = []

    def dispatch(first, total):
        total = jnp.concatenate([total[:T], total[T:]], axis=1)
        for at in range(0, wide, step):
            cols = slice(first + at, first + at + step)
            hidden = base[:, cols] + total[:, at:at + step]
            hs[:, cols] = hidden
            stacked = jnp.concatenate(
                [hidden[:, p * piece:(p + 1) * piece] for p in range(Q)], axis=0
            ).astype(BF16)
            picked = lax.dot_general(
                table, stacked, (((0,), (0,)), ((), ())), preferred_element_type=F32
            ).astype(BF16)
            k = len(x_x)
            xb[k] = picked
            for m in far_first:
                to_peer(
                    xb.at[k, rows_at(m, 1)], xr.at[k, rows_at(m, 1)], sx.at[k], rx.at[k], m
                ).start()
            xr[k, 0:TILE] = picked[0:TILE]
            x_x.append(whole(xr.at[k, rows_at(1, E - 1)], sx.at[k], rx.at[k]))

    a_all = whole(rsa.at[rows_at(1, E - 1)], sa.at[0], ra.at[0])
    a_all.wait_recv()
    total = ya[0:TILE, :].astype(F32)
    for m in range(1, E):
        total = total + rsa[m * TILE:(m + 1) * TILE, :].astype(F32)
    dispatch(0, total)
    c_all = whole(rsc.at[rows_at(1, O - 1)], sc.at[0], rc.at[0])
    c_all.wait_recv()
    total = kept
    for o in outer:
        total = total + rsc[o * TILE:(o + 1) * TILE, :].astype(F32)
    dispatch(wide, total)

    for cp in wcopies[2:]:
        cp.wait()
    wg_x.wait()
    wu_x.wait()
    wd_x.wait()
    for cp in (a_all, b_all, c_all):
        cp.wait_send()
    px = parts_out(Q, cap)
    gc = 8 * cap
    rows = E * cap
    gain = gain_ref[mine].astype(F32).reshape(1, half)
    square = jnp.zeros((rows, 1), F32)
    F = 2 * FH
    gates, ups = slice(128, 128 + F), slice(128 + F, 128 + 2 * F)
    for k in range(C):
        x_x[k].wait_recv()
        blk = [
            dot(px, xr[k, grp * 8 * TILE:(grp + 1) * 8 * TILE, :]) for grp in range(E // 8)
        ]
        for p in range(Q):
            part = jnp.concatenate([v[p * gc:(p + 1) * gc] for v in blk], axis=0)
            square = square + jnp.sum(part * part, axis=1, keepdims=True)
            cols = slice(k * step + p * piece, k * step + (p + 1) * piece)
            xs[:, cols] = (part * gain[:, cols]).astype(BF16)
        feats = slice(k * step, (k + 1) * step)
        if k == 0:
            gus[:, gates] = dot(xs[:, feats], wg[feats, :])
        else:
            gus[:, gates] += dot(xs[:, feats], wg[feats, :])
        if k == C - 1:
            gus[:, 0:128] = jnp.broadcast_to(square, (rows, 128))
            first = pl.ds(0, 128 + F)
            g_x = beside(gus.at[:, first], gur.at[:, first], 5)
            g_x.start()
        if k == 0:
            gus[:, ups] = dot(xs[:, feats], wu[feats, :])
        else:
            gus[:, ups] += dot(xs[:, feats], wu[feats, :])
    second = pl.ds(128 + F, F)
    u_x = beside(gus.at[:, second], gur.at[:, second], 6)
    u_x.start()
    g_x.wait()
    scale = lax.rsqrt((gus[:, 0:1] + gur[:, 0:1]) / D + 1e-06)
    gate = (gus[:, 128:128 + F] + gur[:, 128:128 + F]) * scale
    gate = gate / (1.0 + jnp.exp(-gate))
    u_x.wait()
    up = (gus[:, 128 + F:128 + 2 * F] + gur[:, 128 + F:128 + 2 * F]) * scale
    hid[...] = (gate * up).astype(BF16)

    pb = parts_in(Q, cap)
    z_x = []
    for k in range(C):
        o = dot(hid[...], wd[:, k * step:(k + 1) * step]).astype(BF16)
        for grp in range(E // 8):
            blk = jnp.concatenate([
                o[grp * gc:(grp + 1) * gc, p * piece:(p + 1) * piece] for p in range(Q)
            ], axis=0)
            zs[k, grp * 8 * TILE:(grp + 1) * 8 * TILE, :] = dot(pb, blk).astype(BF16)
        for m in far_first:
            to_peer(
                zs.at[k, rows_at(m, 1)], zr.at[k, rows_at(m, 1)], sz.at[k], rz.at[k], m
            ).start()
        zr[k, 0:TILE] = zs[k, 0:TILE]
        z_x.append(whole(zr.at[k, rows_at(1, E - 1)], sz.at[k], rz.at[k]))

    for cp in x_x:
        cp.wait_send()
    wh = whi[...].astype(BF16)
    wl = wlo[...].astype(BF16)
    own = c == 0
    f_x = []
    for k in range(C):
        z_x[k].wait_recv()
        part = dot(wh, zr[k]) + dot(wl, zr[k])
        cols = slice(k * step, (k + 1) * step)
        updated = hs[:, cols] + jnp.concatenate(
            [part[p * T:(p + 1) * T] for p in range(Q)], axis=1
        )
        ub[:, cols] = updated
        f_x.append(beside(ub.at[:, pl.ds(k * step, step)], up_.at[:, pl.ds(k * step, step)], 7 + k))
        f_x[k].start()
        at = pl.ds(pl.multiple_of(c * half + k * step, step), step)
        out_ref[:, at] = jnp.where(own, updated[:S], updated[S:]).astype(BF16)
    for cp in z_x:
        cp.wait_send()
    for cp in f_x:
        cp.wait()
    got = up_[...]
    out_ref[:, other] = jnp.where(own, got[:S], got[S:]).astype(BF16)


def on_device(
    queries, token_keys, token_values, stored_keys, stored_values, kv_len, residual, out_weight,
    norm_gain, expert_ids, route_weight, w_gate, w_up, w_down,
):
    E = lax.axis_size("expert")
    N = 2 * E
    I = 1 << ((E.bit_length() - 1) // 2)
    O = E // I
    S, features = queries.shape
    T = 2 * S
    L = stored_keys.shape[1]
    KW = token_keys.shape[1]
    D = residual.shape[1]
    half = D // 2
    wide = half // 2
    topk = expert_ids.shape[1]
    FH = w_gate.shape[2]
    cap = max(2, -(-(T * topk) // E))
    Q = TILE // cap
    piece = HEAD_WIDTH
    C = half // (Q * piece)
    orow = out_weight.shape[0]
    hbm = pl.BlockSpec(memory_space=pltpu.HBM)
    V = pltpu.VMEM
    dma = pltpu.SemaphoreType.DMA
    wout = 128 + 4 * FH
    scratch = [
        V((S, features), BF16), V((S, KW), BF16), V((S, KW), BF16), pltpu.SMEM((S,), jnp.int32),
        V((S, D), BF16), V((D,), BF16), V(expert_ids.shape, jnp.int32), V(route_weight.shape, F32),
        V((S, L, KW), BF16), V((S, L, KW), BF16),
        V((orow, half), BF16), V((2 * orow, half), BF16),
        V((half, 2 * FH), BF16), V((half, 2 * FH), BF16), V((2 * FH, half), BF16),
        V((S * features // HEAD_WIDTH, HEAD_WIDTH), F32), V((8, KW), F32), V((8, KW), F32),
        V((E * TILE, HEAD_WIDTH), F32), V((E * TILE, HEAD_WIDTH), BF16),
        V((N * TILE, HEAD_WIDTH), BF16), V((N * S, 2 * orow), BF16),
        V((E * TILE, wide // 2), BF16), V((E * TILE, wide // 2), BF16),
        V((E * TILE, wide // 2), BF16), V((I, O * TILE, wide // 2), BF16),
        V((O * TILE, wide // 2), BF16), V((O * TILE, wide // 2), BF16),
        V((T, D), F32), V((T, half), F32), V((T, half), F32),
        V((Q * T, E * TILE), F32), V((Q * T, E * TILE), F32), V((Q * T, E * TILE), F32),
        V((C, E * TILE, piece), BF16), V((C, E * TILE, piece), BF16), V((E * cap, half), BF16),
        V((E * cap, wout), F32), V((E * cap, wout), F32), V((E * cap, 2 * FH), BF16),
        V((C, E * TILE, piece), BF16), V((C, E * TILE, piece), BF16),
        V((T, half), F32), V((T, half), F32),
        dma((8,)), dma((2,)), dma((5,)), dma((7 + C,)), dma((7 + C,)),
        *[dma((1,))] * 8, *[dma((C,))] * 4,
    ]
    return pl.pallas_call(
        functools.partial(kernel, E, I, cap),
        out_shape=pltpu.VMEM((S, D), BF16),
        in_specs=[hbm] * 14,
        out_specs=pl.BlockSpec(memory_space=pltpu.VMEM),
        scratch_shapes=scratch,
        compiler_params=pltpu.CompilerParams(
            collective_id=0, has_side_effects=True, vmem_limit_bytes=66977792
        ),
    )(
        queries, token_keys, token_values, kv_len, residual, norm_gain, expert_ids,
        route_weight, stored_keys, stored_values, out_weight, w_gate, w_up, w_down,
    )


def solution(mesh):
    rows = P(("groups", "expert", "replica"), None)
    cube = P(("groups", "expert", "replica"), None, None)
    in_specs = (
        rows, rows, rows, cube, cube, P(("groups", "expert", "replica")), rows,
        P(("expert", "replica"), None), P(), P(("groups", "expert"), None),
        P(("groups", "expert"), None), P("expert", None, "replica"),
        P("expert", None, "replica"), P("expert", "replica", None),
    )
    return jax.shard_map(
        on_device, mesh=mesh, in_specs=in_specs, out_specs=rows, check_vma=False
    )
```

```python
import functools
import math

import jax
import jax.numpy as jnp
from jax import lax
from jax.experimental import pallas as pl
from jax.experimental.pallas import tpu as pltpu
from jax.sharding import PartitionSpec as P

HEAD_WIDTH = 128
TILE = 16
MESH = pl.DeviceIdType.MESH
F32 = jnp.float32
BF16 = jnp.bfloat16


def permutation(size, source):
    a = lax.broadcasted_iota(jnp.int32, (size, 8 * TILE), 0)
    b = lax.broadcasted_iota(jnp.int32, (size, 8 * TILE), 1)
    return jnp.where(b == source(a), 1.0, 0.0).astype(BF16)


def heads_out(hpc, S):
    return permutation(
        8 * hpc * S,
        lambda a: ((a // S) % 8) * TILE + (a % S) * hpc + a // (8 * S),
    )


def parts_out(Q, cap):
    return permutation(
        8 * Q * cap,
        lambda a: ((a // cap) % 8) * TILE + (a // (8 * cap)) * cap + a % cap,
    )


def parts_in(Q, cap):
    return permutation(
        8 * Q * cap,
        lambda a: ((a % TILE) // cap) * 8 * cap + (a // TILE) * cap + a % cap,
    )


def send_order(C):
    return list(range(C // 2, C)) + list(range(C // 2))


def dot(a, b):
    return jnp.dot(a, b, preferred_element_type=F32)


def kernel(
    E, I, cap,
    q_hbm, tk_hbm, tv_hbm, kv_hbm, res_hbm, gain_hbm, ids_hbm, rw_hbm,
    k_hbm, v_hbm, ow_hbm, wg_hbm, wu_hbm, wd_hbm,
    out_ref,
    q_ref, tk_ref, tv_ref, kv_ref, res_ref, gain_ref, ids_ref, rw_ref,
    kb, vb, owo, ow, wg, wu, wd,
    qs, tks, tvs, attf, att, ratt, asm,
    ys, rsa, rsb, zb, rsc,
    resb, resp, hs, tts, whi, wlo,
    xb, xr, xs, gus, gur, hid, zs, zr, ub, up_,
    isem, ksem, wsem, psend, precv,
    s1, r1, sa, ra, sb, rb, sc, rc, sx, rx, sz, rz,
):
    N = 2 * E
    O = E // I
    bits = E.bit_length() - 1
    e_me = lax.axis_index("expert")
    c = lax.axis_index("replica")
    rank = e_me * 2 + c
    S = q_ref.shape[0]
    T = 2 * S
    heads = q_ref.shape[1] // HEAD_WIDTH
    G = tk_ref.shape[1] // HEAD_WIDTH
    width = heads // G
    L = k_hbm.shape[1]
    D = res_ref.shape[1]
    half = D // 2
    hpc = heads // E
    Q = TILE // cap
    piece = HEAD_WIDTH
    step = Q * piece
    C = half // step
    FH = wg_hbm.shape[2]
    orow = ow_hbm.shape[0]
    drow = wd_hbm.shape[1]
    mine = pl.ds(pl.multiple_of(c * half, half), half)
    other = pl.ds(pl.multiple_of((1 - c) * half, half), half)
    omine = pl.ds(pl.multiple_of(c * orow, orow), orow)
    dmine = pl.ds(pl.multiple_of(c * drow, drow), drow)
    fmine = pl.ds(pl.multiple_of(c * FH, FH), FH)

    place = []
    for k in range(bits):
        bit = lax.rem(lax.div(e_me, 1 << k), 2)
        place.append((bit * (1 << k), (1 - bit) * (1 << k)))

    def expert_at(mask):
        return functools.reduce(lambda a, b: a + b, [place[k][(mask >> k) & 1] for k in range(bits)])

    peer = [expert_at(m) for m in range(E)]
    side = [c, 1 - c]
    order = {m: (m % I) * O + m // I for m in range(E)}

    small = [
        pltpu.make_async_copy(src, dst, isem.at[k])
        for k, (src, dst) in enumerate((
            (q_hbm, q_ref), (tk_hbm, tk_ref), (tv_hbm, tv_ref), (kv_hbm, kv_ref),
            (res_hbm, res_ref), (gain_hbm, gain_ref), (ids_hbm, ids_ref), (rw_hbm, rw_ref),
        ))
    ]
    k_copy = pltpu.make_async_copy(k_hbm, kb, ksem.at[0])
    v_copy = pltpu.make_async_copy(v_hbm, vb, ksem.at[1])
    wcopies = [
        pltpu.make_async_copy(ow_hbm.at[:, other], owo, wsem.at[0]),
        pltpu.make_async_copy(ow_hbm.at[:, mine], ow.at[omine], wsem.at[1]),
        pltpu.make_async_copy(wg_hbm.at[0, mine], wg.at[:, fmine], wsem.at[2]),
        pltpu.make_async_copy(wu_hbm.at[0, mine], wu.at[:, fmine], wsem.at[3]),
        pltpu.make_async_copy(wd_hbm.at[0, :, mine], wd.at[dmine], wsem.at[4]),
    ]
    for cp in small[:4] + [k_copy, v_copy]:
        cp.start()
    barrier = pltpu.get_barrier_semaphore()
    for m in range(E - 1, -1, -1):
        for k in (0, 1):
            if m or k:
                pl.semaphore_signal(
                    barrier, inc=1,
                    device_id={"expert": peer[m], "replica": side[k]}, device_id_type=MESH,
                )
    for cp in small[4:]:
        cp.start()

    for cp in small[:4]:
        cp.wait()
    qf = q_ref[...].astype(F32)
    for h in range(heads):
        qs[pl.ds(S * h, S), :] = qf[:, h * HEAD_WIDTH:(h + 1) * HEAD_WIDTH]
    tks[0:S, :] = tk_ref[...].astype(F32)
    tvs[0:S, :] = tv_ref[...].astype(F32)
    if hpc * S < TILE:
        attf[...] = jnp.zeros_like(attf)
    inv_root = 1.0 / math.sqrt(HEAD_WIDTH)
    group = lax.broadcasted_iota(jnp.int32, (heads, HEAD_WIDTH), 0) // width
    col = lax.broadcasted_iota(jnp.int32, (heads, L), 1)

    def by_head(ref, b):
        return jnp.concatenate([
            jnp.broadcast_to(ref[b:b + 1, g * HEAD_WIDTH:(g + 1) * HEAD_WIDTH], (width, HEAD_WIDTH))
            for g in range(G)
        ], axis=0)

    rows_q = []
    fresh = []
    for b in range(S):
        qb = qs[pl.ds(b, heads, stride=S), :]
        rows_q.append(jnp.concatenate(
            [jnp.where(group == g, qb, 0.0).astype(BF16) for g in range(G)], axis=1
        ))
        fresh.append(jnp.sum(qb * by_head(tks, b), axis=1, keepdims=True) * inv_root)
    k_copy.wait()
    probs = []
    fprobs = []
    for b in range(S):
        score = lax.dot_general(
            rows_q[b], kb[b], (((1,), (1,)), ((), ())),
            preferred_element_type=F32,
        ) * inv_root
        score = jnp.where(col < kv_ref[b], score, -jnp.inf)
        top = jnp.maximum(jnp.max(score, axis=1, keepdims=True), fresh[b])
        ex = jnp.exp(score - top)
        fex = jnp.exp(fresh[b] - top)
        inv = 1.0 / (jnp.sum(ex, axis=1, keepdims=True) + fex)
        probs.append((ex * inv).astype(BF16))
        fprobs.append((fex * inv).astype(BF16).astype(F32))
    v_copy.wait()
    for cp in wcopies:
        cp.start()
    for b in range(S):
        o = dot(probs[b], vb[b])
        o = jnp.concatenate([
            o[g * width:(g + 1) * width, g * HEAD_WIDTH:(g + 1) * HEAD_WIDTH] for g in range(G)
        ], axis=0)
        o = o + fprobs[b] * by_head(tvs, b)
        for j in range(E):
            attf[j * TILE + b * hpc:j * TILE + (b + 1) * hpc, :] = o[j * hpc:(j + 1) * hpc]
    att[...] = attf[...].astype(BF16)

    pl.semaphore_wait(barrier, N - 1)

    def rows_at(start, count):
        return pl.ds(pl.multiple_of(start * TILE, TILE), count * TILE)

    def att_copy(m, k):
        return pltpu.make_async_remote_copy(
            src_ref=att.at[rows_at(peer[m], 1)], dst_ref=ratt.at[rows_at(2 * order[m] + c, 1)],
            send_sem=s1.at[0], recv_sem=r1.at[0],
            device_id={"expert": peer[m], "replica": side[k]}, device_id_type=MESH,
        )

    def to_peer(src, dst, send, recv, m):
        return pltpu.make_async_remote_copy(
            src_ref=src, dst_ref=dst, send_sem=send, recv_sem=recv,
            device_id={"expert": peer[m], "replica": c}, device_id_type=MESH,
        )

    def beside(src, dst, k):
        return pltpu.make_async_remote_copy(
            src_ref=src, dst_ref=dst, send_sem=psend.at[k], recv_sem=precv.at[k],
            device_id={"expert": e_me, "replica": 1 - c}, device_id_type=MESH,
        )

    def whole(ref, send, recv):
        return to_peer(ref, ref, send, recv, E - 1)

    far_first = range(E - 1, 0, -1)
    att_x = [att_copy(m, k) for m in far_first for k in (0, 1)] + [att_copy(0, 1)]
    for cp in att_x:
        cp.start()
    att_all = whole(ratt.at[rows_at(0, N - 1)], s1.at[0], r1.at[0])
    wcopies[0].wait()
    wg_x = beside(wg_hbm.at[0, other], wg.at[:, fmine], 2)
    wu_x = beside(wu_hbm.at[0, other], wu.at[:, fmine], 3)
    wd_x = beside(wd_hbm.at[0, :, other], wd.at[dmine], 4)
    ow_x = beside(owo, ow.at[omine], 0)
    ow_x.start()
    for cp in (wg_x, wu_x, wd_x):
        cp.start()
    for cp in small[4:]:
        cp.wait()
    ratt[rows_at(c, 1)] = att[rows_at(e_me, 1)]
    for rep in range(8 // S):
        resb[pl.ds(rep * S, S), :] = res_ref[...].astype(F32)
    res_x = beside(resb.at[:, other], resp, 1)
    res_x.start()

    lanes_all = E * TILE
    lane = lax.broadcasted_iota(jnp.int32, (T, lanes_all), 1)
    tok = lax.broadcasted_iota(jnp.int32, (T, lanes_all), 0)
    lm = lane // TILE
    le = jnp.zeros((T, lanes_all), jnp.int32)
    for k in range(bits):
        flip = (lm // (1 << k)) % 2
        le = le + jnp.where(flip == 1, place[k][1], place[k][0])
    lq = (lane // cap) % Q
    ls = lane % cap
    ids = ids_ref[...]
    rw = rw_ref[...]
    mix = rw / jnp.sum(rw, axis=1, keepdims=True)
    named = jnp.zeros((T, lanes_all), F32)
    weight = jnp.zeros((T, lanes_all), F32)
    for k in range(ids.shape[1]):
        hit = ids[:, k:k + 1] == le
        named = named + jnp.where(hit, 1.0, 0.0)
        weight = weight + jnp.where(hit, mix[:, k:k + 1], 0.0)
    before = jnp.zeros((T, lanes_all), F32)
    for t in range(T - 1):
        before = before + jnp.where(tok > t, named[t:t + 1, :], 0.0)
    chosen = jnp.where(before == ls.astype(F32), named, 0.0)
    weight = weight * chosen
    high = weight.astype(BF16).astype(F32)
    low = weight - high
    for p in range(Q):
        here = lq == p
        tts[p * T:(p + 1) * T, :] = jnp.where(here, chosen, 0.0)
        whi[p * T:(p + 1) * T, :] = jnp.where(here, high, 0.0)
        wlo[p * T:(p + 1) * T, :] = jnp.where(here, low, 0.0)

    wcopies[1].wait()
    ow_x.wait()
    att_all.wait_recv()

    pa = heads_out(hpc, S)
    for grp in range(N // 8):
        blk = dot(pa, ratt[grp * 8 * TILE:(grp + 1) * 8 * TILE, :]).astype(BF16)
        for h in range(hpc):
            asm[grp * 8 * S:(grp + 1) * 8 * S, h * HEAD_WIDTH:(h + 1) * HEAD_WIDTH] = (
                blk[h * 8 * S:(h + 1) * 8 * S]
            )
    lanes = step // 2
    direct = C // 2
    inner = range(I - 1, 0, -1)
    outer = range(O - 1, 0, -1)
    for k in send_order(C):
        y = [
            dot(asm[...], ow[:, k * step + j * lanes:k * step + (j + 1) * lanes]) for j in (0, 1)
        ]
        both = jnp.concatenate([v.reshape(E, T, lanes) for v in y], axis=1)
        ys[k] = both.reshape(E * TILE, lanes).astype(BF16)
        if k < direct:
            for m in far_first:
                to_peer(
                    ys.at[k, rows_at(order[m], 1)], rsa.at[k, rows_at(order[m], 1)],
                    sa.at[k], ra.at[k], m,
                ).start()
        else:
            b = k - direct
            for p in inner:
                to_peer(
                    ys.at[k, rows_at(p * O, O)], rsb.at[b, p], sb.at[b], rb.at[b], p
                ).start()
    a_x = [whole(rsa.at[k, rows_at(1, E - 1)], sa.at[k], ra.at[k]) for k in range(direct)]
    b_x = [whole(rsb.at[b, pl.ds(1, I - 1)], sb.at[b], rb.at[b]) for b in range(C - direct)]
    c_x = [whole(rsc.at[b, rows_at(1, O - 1)], sc.at[b], rc.at[b]) for b in range(C - direct)]
    kept = []
    for b in range(C - direct):
        b_x[b].wait_recv()
        relay = ys[direct + b, 0:O * TILE, :].astype(F32)
        for p in range(1, I):
            relay = relay + rsb[b, p].astype(F32)
        zb[b] = relay.astype(BF16)
        kept.append(relay[0:TILE])
        for o in outer:
            to_peer(
                zb.at[b, rows_at(o, 1)], rsc.at[b, rows_at(o, 1)], sc.at[b], rc.at[b], o * I
            ).start()

    res_x.wait()
    att_all.wait_send()
    trow = lax.broadcasted_iota(jnp.int32, (T, half), 0)
    base = jnp.where(trow // S == c, resb[:, mine], resp[...])
    table = tts[...].astype(BF16)

    x_x = []

    def dispatch(k, total):
        cols = slice(k * step, (k + 1) * step)
        hidden = base[:, cols] + jnp.concatenate([total[:T], total[T:]], axis=1)
        hs[:, cols] = hidden
        stacked = jnp.concatenate(
            [hidden[:, p * piece:(p + 1) * piece] for p in range(Q)], axis=0
        ).astype(BF16)
        picked = lax.dot_general(
            table, stacked, (((0,), (0,)), ((), ())), preferred_element_type=F32
        ).astype(BF16)
        xb[k] = picked
        for m in far_first:
            to_peer(
                xb.at[k, rows_at(m, 1)], xr.at[k, rows_at(m, 1)], sx.at[k], rx.at[k], m
            ).start()
        xr[k, 0:TILE] = picked[0:TILE]
        x_x.append(whole(xr.at[k, rows_at(1, E - 1)], sx.at[k], rx.at[k]))

    for k in range(direct):
        a_x[k].wait_recv()
        total = ys[k, 0:TILE, :].astype(F32)
        for m in range(1, E):
            total = total + rsa[k, m * TILE:(m + 1) * TILE, :].astype(F32)
        dispatch(k, total)
    for b in range(C - direct):
        c_x[b].wait_recv()
        total = kept[b]
        for o in range(1, O):
            total = total + rsc[b, o * TILE:(o + 1) * TILE, :].astype(F32)
        dispatch(direct + b, total)

    for cp in wcopies[2:]:
        cp.wait()
    wg_x.wait()
    wu_x.wait()
    wd_x.wait()
    for cp in a_x + b_x + c_x:
        cp.wait_send()
    px = parts_out(Q, cap)
    gc = 8 * cap
    rows = E * cap
    gain = gain_ref[mine].astype(F32).reshape(1, half)
    square = jnp.zeros((rows, 1), F32)
    F = 2 * FH
    gates, ups = slice(128, 128 + F), slice(128 + F, 128 + 2 * F)
    for k in range(C):
        x_x[k].wait_recv()
        blk = [
            dot(px, xr[k, grp * 8 * TILE:(grp + 1) * 8 * TILE, :]) for grp in range(E // 8)
        ]
        for p in range(Q):
            part = jnp.concatenate([v[p * gc:(p + 1) * gc] for v in blk], axis=0)
            square = square + jnp.sum(part * part, axis=1, keepdims=True)
            cols = slice(k * step + p * piece, k * step + (p + 1) * piece)
            xs[:, cols] = (part * gain[:, cols]).astype(BF16)
        feats = slice(k * step, (k + 1) * step)
        if k == 0:
            gus[:, gates] = dot(xs[:, feats], wg[feats, :])
        else:
            gus[:, gates] += dot(xs[:, feats], wg[feats, :])
        if k == C - 1:
            gus[:, 0:128] = jnp.broadcast_to(square, (rows, 128))
            first = pl.ds(0, 128 + F)
            g_x = beside(gus.at[:, first], gur.at[:, first], 5)
            g_x.start()
        if k == 0:
            gus[:, ups] = dot(xs[:, feats], wu[feats, :])
        else:
            gus[:, ups] += dot(xs[:, feats], wu[feats, :])
    second = pl.ds(128 + F, F)
    u_x = beside(gus.at[:, second], gur.at[:, second], 6)
    u_x.start()
    g_x.wait()
    scale = lax.rsqrt((gus[:, 0:1] + gur[:, 0:1]) / D + 1e-06)
    gate = (gus[:, 128:128 + F] + gur[:, 128:128 + F]) * scale
    gate = gate / (1.0 + jnp.exp(-gate))
    u_x.wait()
    up = (gus[:, 128 + F:128 + 2 * F] + gur[:, 128 + F:128 + 2 * F]) * scale
    hid[...] = (gate * up).astype(BF16)

    pb = parts_in(Q, cap)
    z_x = []
    for k in range(C):
        o = dot(hid[...], wd[:, k * step:(k + 1) * step]).astype(BF16)
        for grp in range(E // 8):
            blk = jnp.concatenate([
                o[grp * gc:(grp + 1) * gc, p * piece:(p + 1) * piece] for p in range(Q)
            ], axis=0)
            zs[k, grp * 8 * TILE:(grp + 1) * 8 * TILE, :] = dot(pb, blk).astype(BF16)
        for m in far_first:
            to_peer(
                zs.at[k, rows_at(m, 1)], zr.at[k, rows_at(m, 1)], sz.at[k], rz.at[k], m
            ).start()
        zr[k, 0:TILE] = zs[k, 0:TILE]
        z_x.append(whole(zr.at[k, rows_at(1, E - 1)], sz.at[k], rz.at[k]))

    for cp in x_x:
        cp.wait_send()
    wh = whi[...].astype(BF16)
    wl = wlo[...].astype(BF16)
    own = c == 0
    f_x = []
    for k in range(C):
        z_x[k].wait_recv()
        part = dot(wh, zr[k]) + dot(wl, zr[k])
        cols = slice(k * step, (k + 1) * step)
        updated = hs[:, cols] + jnp.concatenate(
            [part[p * T:(p + 1) * T] for p in range(Q)], axis=1
        )
        ub[:, cols] = updated
        f_x.append(beside(ub.at[:, pl.ds(k * step, step)], up_.at[:, pl.ds(k * step, step)], 7 + k))
        f_x[k].start()
        at = pl.ds(pl.multiple_of(c * half + k * step, step), step)
        out_ref[:, at] = jnp.where(own, updated[:S], updated[S:]).astype(BF16)
    for cp in z_x:
        cp.wait_send()
    for cp in f_x:
        cp.wait()
    got = up_[...]
    out_ref[:, other] = jnp.where(own, got[:S], got[S:]).astype(BF16)


def on_device(
    queries, token_keys, token_values, stored_keys, stored_values, kv_len, residual, out_weight,
    norm_gain, expert_ids, route_weight, w_gate, w_up, w_down,
):
    E = lax.axis_size("expert")
    N = 2 * E
    I = 1 << ((E.bit_length() - 1) // 2)
    O = E // I
    S, features = queries.shape
    T = 2 * S
    L = stored_keys.shape[1]
    KW = token_keys.shape[1]
    D = residual.shape[1]
    half = D // 2
    topk = expert_ids.shape[1]
    FH = w_gate.shape[2]
    cap = max(2, -(-(T * topk) // E))
    Q = TILE // cap
    piece = HEAD_WIDTH
    C = half // (Q * piece)
    A = C // 2
    B = C - A
    lanes = half // C // 2
    orow = out_weight.shape[0]
    hbm = pl.BlockSpec(memory_space=pltpu.HBM)
    V = pltpu.VMEM
    dma = pltpu.SemaphoreType.DMA
    wout = 128 + 4 * FH
    scratch = [
        V((S, features), BF16), V((S, KW), BF16), V((S, KW), BF16), pltpu.SMEM((S,), jnp.int32),
        V((S, D), BF16), V((D,), BF16), V(expert_ids.shape, jnp.int32), V(route_weight.shape, F32),
        V((S, L, KW), BF16), V((S, L, KW), BF16),
        V((orow, half), BF16), V((2 * orow, half), BF16),
        V((half, 2 * FH), BF16), V((half, 2 * FH), BF16), V((2 * FH, half), BF16),
        V((S * features // HEAD_WIDTH, HEAD_WIDTH), F32), V((8, KW), F32), V((8, KW), F32),
        V((E * TILE, HEAD_WIDTH), F32), V((E * TILE, HEAD_WIDTH), BF16),
        V((N * TILE, HEAD_WIDTH), BF16), V((N * S, 2 * orow), BF16),
        V((C, E * TILE, lanes), BF16), V((A, E * TILE, lanes), BF16),
        V((B, I, O * TILE, lanes), BF16), V((B, O * TILE, lanes), BF16), V((B, O * TILE, lanes), BF16),
        V((T, D), F32), V((T, half), F32), V((T, half), F32),
        V((Q * T, E * TILE), F32), V((Q * T, E * TILE), F32), V((Q * T, E * TILE), F32),
        V((C, E * TILE, piece), BF16), V((C, E * TILE, piece), BF16), V((E * cap, half), BF16),
        V((E * cap, wout), F32), V((E * cap, wout), F32), V((E * cap, 2 * FH), BF16),
        V((C, E * TILE, piece), BF16), V((C, E * TILE, piece), BF16),
        V((T, half), F32), V((T, half), F32),
        dma((8,)), dma((2,)), dma((5,)), dma((7 + C,)), dma((7 + C,)),
        *[dma((1,))] * 2, *[dma((A,))] * 2, *[dma((B,))] * 4, *[dma((C,))] * 4,
    ]
    return pl.pallas_call(
        functools.partial(kernel, E, I, cap),
        out_shape=pltpu.VMEM((S, D), BF16),
        in_specs=[hbm] * 14,
        out_specs=pl.BlockSpec(memory_space=pltpu.VMEM),
        scratch_shapes=scratch,
        compiler_params=pltpu.CompilerParams(
            collective_id=0, has_side_effects=True, vmem_limit_bytes=66977792
        ),
    )(
        queries, token_keys, token_values, kv_len, residual, norm_gain, expert_ids,
        route_weight, stored_keys, stored_values, out_weight, w_gate, w_up, w_down,
    )


def solution(mesh):
    rows = P(("groups", "expert", "replica"), None)
    cube = P(("groups", "expert", "replica"), None, None)
    in_specs = (
        rows, rows, rows, cube, cube, P(("groups", "expert", "replica")), rows,
        P(("expert", "replica"), None), P(), P(("groups", "expert"), None),
        P(("groups", "expert"), None), P("expert", None, "replica"),
        P("expert", None, "replica"), P("expert", "replica", None),
    )
    return jax.shard_map(
        on_device, mesh=mesh, in_specs=in_specs, out_specs=rows, check_vma=False
    )
```

```python
import functools
import math

import jax
import jax.numpy as jnp
from jax import lax
from jax.experimental import pallas as pl
from jax.experimental.pallas import tpu as pltpu
from jax.sharding import PartitionSpec as P

HEAD_WIDTH = 128
TILE = 16
CHUNKS = 4
RETURNS = 2
MESH = pl.DeviceIdType.MESH
F32 = jnp.float32
BF16 = jnp.bfloat16


def permutation(size, source):
    a = lax.broadcasted_iota(jnp.int32, (size, 8 * TILE), 0)
    b = lax.broadcasted_iota(jnp.int32, (size, 8 * TILE), 1)
    return jnp.where(b == source(a), 1.0, 0.0).astype(BF16)


def heads_out(hpc, S):
    return permutation(
        8 * hpc * S,
        lambda a: ((a // S) % 8) * TILE + (a % S) * hpc + a // (8 * S),
    )


def dot(a, b):
    return jnp.dot(a, b, preferred_element_type=F32)


def kernel(
    E, I, cap, C, direct, Z,
    q_hbm, tk_hbm, tv_hbm, kv_hbm, res_hbm, gain_hbm, ids_hbm, rw_hbm,
    k_hbm, v_hbm, ow_hbm, wg_hbm, wu_hbm, wd_hbm,
    out_ref,
    q_ref, tk_ref, tv_ref, kv_ref, res_ref, gain_ref, ids_ref, rw_ref,
    kb, vb, owo, ow, wg, wu, wd,
    qs, tks, tvs, attf, att, ratt, asm,
    ys, rsa, rsb, zb, rsc,
    resb, resp, hs, tts, whi, wlo,
    xb, xr, xs, gus, gur, hid, zs, zr, ub, up_,
    isem, ksem, wsem, psend, precv,
    s1, r1, sa, ra, sb, rb, sc, rc, sx, rx, sz, rz,
):
    N = 2 * E
    O = E // I
    bits = E.bit_length() - 1
    e_me = lax.axis_index("expert")
    c = lax.axis_index("replica")
    rank = e_me * 2 + c
    S = q_ref.shape[0]
    T = 2 * S
    heads = q_ref.shape[1] // HEAD_WIDTH
    G = tk_ref.shape[1] // HEAD_WIDTH
    width = heads // G
    L = k_hbm.shape[1]
    D = res_ref.shape[1]
    half = D // 2
    hpc = heads // E
    step = half // C
    FH = wg_hbm.shape[2]
    orow = ow_hbm.shape[0]
    drow = wd_hbm.shape[1]
    mine = pl.ds(pl.multiple_of(c * half, half), half)
    other = pl.ds(pl.multiple_of((1 - c) * half, half), half)
    omine = pl.ds(pl.multiple_of(c * orow, orow), orow)
    dmine = pl.ds(pl.multiple_of(c * drow, drow), drow)
    fmine = pl.ds(pl.multiple_of(c * FH, FH), FH)

    place = []
    for k in range(bits):
        bit = lax.rem(lax.div(e_me, 1 << k), 2)
        place.append((bit * (1 << k), (1 - bit) * (1 << k)))

    def expert_at(mask):
        return functools.reduce(lambda a, b: a + b, [place[k][(mask >> k) & 1] for k in range(bits)])

    peer = [expert_at(m) for m in range(E)]
    side = [c, 1 - c]
    order = {m: (m % I) * O + m // I for m in range(E)}

    small = [
        pltpu.make_async_copy(src, dst, isem.at[k])
        for k, (src, dst) in enumerate((
            (q_hbm, q_ref), (tk_hbm, tk_ref), (tv_hbm, tv_ref), (kv_hbm, kv_ref),
            (res_hbm, res_ref), (gain_hbm, gain_ref), (ids_hbm, ids_ref), (rw_hbm, rw_ref),
        ))
    ]
    k_copy = pltpu.make_async_copy(k_hbm, kb, ksem.at[0])
    v_copy = pltpu.make_async_copy(v_hbm, vb, ksem.at[1])
    wcopies = [
        pltpu.make_async_copy(ow_hbm.at[:, other], owo, wsem.at[0]),
        pltpu.make_async_copy(ow_hbm.at[:, mine], ow.at[omine], wsem.at[1]),
        pltpu.make_async_copy(wg_hbm.at[0, mine], wg.at[:, fmine], wsem.at[2]),
        pltpu.make_async_copy(wu_hbm.at[0, mine], wu.at[:, fmine], wsem.at[3]),
        pltpu.make_async_copy(wd_hbm.at[0, :, mine], wd.at[dmine], wsem.at[4]),
    ]
    for cp in small[:4] + [k_copy, v_copy]:
        cp.start()
    barrier = pltpu.get_barrier_semaphore()
    for m in range(E - 1, -1, -1):
        for k in (0, 1):
            if m or k:
                pl.semaphore_signal(
                    barrier, inc=1,
                    device_id={"expert": peer[m], "replica": side[k]}, device_id_type=MESH,
                )
    for cp in small[4:]:
        cp.start()

    for cp in small[:4]:
        cp.wait()
    qf = q_ref[...].astype(F32)
    for h in range(heads):
        qs[pl.ds(S * h, S), :] = qf[:, h * HEAD_WIDTH:(h + 1) * HEAD_WIDTH]
    tks[0:S, :] = tk_ref[...].astype(F32)
    tvs[0:S, :] = tv_ref[...].astype(F32)
    if hpc * S < TILE:
        attf[...] = jnp.zeros_like(attf)
    inv_root = 1.0 / math.sqrt(HEAD_WIDTH)
    group = lax.broadcasted_iota(jnp.int32, (heads, HEAD_WIDTH), 0) // width
    col = lax.broadcasted_iota(jnp.int32, (heads, L), 1)

    def by_head(ref, b):
        return jnp.concatenate([
            jnp.broadcast_to(ref[b:b + 1, g * HEAD_WIDTH:(g + 1) * HEAD_WIDTH], (width, HEAD_WIDTH))
            for g in range(G)
        ], axis=0)

    rows_q = []
    fresh = []
    for b in range(S):
        qb = qs[pl.ds(b, heads, stride=S), :]
        rows_q.append(jnp.concatenate(
            [jnp.where(group == g, qb, 0.0).astype(BF16) for g in range(G)], axis=1
        ))
        fresh.append(jnp.sum(qb * by_head(tks, b), axis=1, keepdims=True) * inv_root)
    k_copy.wait()
    probs = []
    fprobs = []
    for b in range(S):
        score = lax.dot_general(
            rows_q[b], kb[b], (((1,), (1,)), ((), ())),
            preferred_element_type=F32,
        ) * inv_root
        score = jnp.where(col < kv_ref[b], score, -jnp.inf)
        top = jnp.maximum(jnp.max(score, axis=1, keepdims=True), fresh[b])
        ex = jnp.exp(score - top)
        fex = jnp.exp(fresh[b] - top)
        inv = 1.0 / (jnp.sum(ex, axis=1, keepdims=True) + fex)
        probs.append((ex * inv).astype(BF16))
        fprobs.append((fex * inv).astype(BF16).astype(F32))
    v_copy.wait()
    for cp in wcopies:
        cp.start()
    for b in range(S):
        o = dot(probs[b], vb[b])
        o = jnp.concatenate([
            o[g * width:(g + 1) * width, g * HEAD_WIDTH:(g + 1) * HEAD_WIDTH] for g in range(G)
        ], axis=0)
        o = o + fprobs[b] * by_head(tvs, b)
        for j in range(E):
            attf[j * TILE + b * hpc:j * TILE + (b + 1) * hpc, :] = o[j * hpc:(j + 1) * hpc]
    att[...] = attf[...].astype(BF16)

    pl.semaphore_wait(barrier, N - 1)

    def rows_at(start, count):
        return pl.ds(pl.multiple_of(start * TILE, TILE), count * TILE)

    def att_copy(m, k):
        return pltpu.make_async_remote_copy(
            src_ref=att.at[rows_at(peer[m], 1)], dst_ref=ratt.at[rows_at(2 * order[m] + c, 1)],
            send_sem=s1.at[0], recv_sem=r1.at[0],
            device_id={"expert": peer[m], "replica": side[k]}, device_id_type=MESH,
        )

    def to_peer(src, dst, send, recv, m):
        return pltpu.make_async_remote_copy(
            src_ref=src, dst_ref=dst, send_sem=send, recv_sem=recv,
            device_id={"expert": peer[m], "replica": c}, device_id_type=MESH,
        )

    def beside(src, dst, k):
        return pltpu.make_async_remote_copy(
            src_ref=src, dst_ref=dst, send_sem=psend.at[k], recv_sem=precv.at[k],
            device_id={"expert": e_me, "replica": 1 - c}, device_id_type=MESH,
        )

    def whole(ref, send, recv):
        return to_peer(ref, ref, send, recv, E - 1)

    far_first = range(E - 1, 0, -1)
    att_x = [att_copy(m, k) for m in far_first for k in (0, 1)] + [att_copy(0, 1)]
    for cp in att_x:
        cp.start()
    att_all = whole(ratt.at[rows_at(0, N - 1)], s1.at[0], r1.at[0])
    wcopies[0].wait()
    wg_x = beside(wg_hbm.at[0, other], wg.at[:, fmine], 2)
    wu_x = beside(wu_hbm.at[0, other], wu.at[:, fmine], 3)
    wd_x = beside(wd_hbm.at[0, :, other], wd.at[dmine], 4)
    ow_x = beside(owo, ow.at[omine], 0)
    ow_x.start()
    for cp in (wg_x, wu_x, wd_x):
        cp.start()
    for cp in small[4:]:
        cp.wait()
    ratt[rows_at(c, 1)] = att[rows_at(e_me, 1)]
    for rep in range(8 // S):
        resb[pl.ds(rep * S, S), :] = res_ref[...].astype(F32)
    res_x = beside(resb.at[:, other], resp, 1)
    res_x.start()

    lanes_all = E * cap
    lane = lax.broadcasted_iota(jnp.int32, (T, lanes_all), 1)
    tok = lax.broadcasted_iota(jnp.int32, (T, lanes_all), 0)
    lm = lane // cap
    le = jnp.zeros((T, lanes_all), jnp.int32)
    for k in range(bits):
        flip = (lm // (1 << k)) % 2
        le = le + jnp.where(flip == 1, place[k][1], place[k][0])
    ls = lane % cap
    ids = ids_ref[...]
    rw = rw_ref[...]
    mix = rw / jnp.sum(rw, axis=1, keepdims=True)
    named = jnp.zeros((T, lanes_all), F32)
    weight = jnp.zeros((T, lanes_all), F32)
    for k in range(ids.shape[1]):
        hit = ids[:, k:k + 1] == le
        named = named + jnp.where(hit, 1.0, 0.0)
        weight = weight + jnp.where(hit, mix[:, k:k + 1], 0.0)
    before = jnp.zeros((T, lanes_all), F32)
    for t in range(T - 1):
        before = before + jnp.where(tok > t, named[t:t + 1, :], 0.0)
    chosen = jnp.where(before == ls.astype(F32), named, 0.0)
    weight = weight * chosen
    high = weight.astype(BF16).astype(F32)
    low = weight - high
    tts[...] = chosen
    whi[...] = high
    wlo[...] = low

    wcopies[1].wait()
    ow_x.wait()
    att_all.wait_recv()

    pa = heads_out(hpc, S)
    for grp in range(N // 8):
        blk = dot(pa, ratt[grp * 8 * TILE:(grp + 1) * 8 * TILE, :]).astype(BF16)
        for h in range(hpc):
            asm[grp * 8 * S:(grp + 1) * 8 * S, h * HEAD_WIDTH:(h + 1) * HEAD_WIDTH] = (
                blk[h * 8 * S:(h + 1) * 8 * S]
            )
    lanes = step // 2
    inner = range(I - 1, 0, -1)
    outer = range(O - 1, 0, -1)
    for k in [*range(direct, C), *range(direct)]:
        y = [
            dot(asm[...], ow[:, k * step + j * lanes:k * step + (j + 1) * lanes]) for j in (0, 1)
        ]
        both = jnp.concatenate([v.reshape(E, T, lanes) for v in y], axis=1)
        ys[k] = both.reshape(E * TILE, lanes).astype(BF16)
        if k < direct:
            for m in far_first:
                to_peer(
                    ys.at[k, rows_at(order[m], 1)], rsa.at[k, rows_at(order[m], 1)],
                    sa.at[0], ra.at[k], m,
                ).start()
        else:
            b = k - direct
            for p in inner:
                to_peer(
                    ys.at[k, rows_at(p * O, O)], rsb.at[b, p], sb.at[0], rb.at[b], p
                ).start()
    a_x = [whole(rsa.at[k, rows_at(1, E - 1)], sa.at[0], ra.at[k]) for k in range(direct)]
    b_x = [whole(rsb.at[b, pl.ds(1, I - 1)], sb.at[0], rb.at[b]) for b in range(C - direct)]
    c_x = [whole(rsc.at[b, rows_at(1, O - 1)], sc.at[0], rc.at[b]) for b in range(C - direct)]
    kept = []
    for b in range(C - direct):
        b_x[b].wait_recv()
        relay = ys[direct + b, 0:O * TILE, :].astype(F32)
        for p in range(1, I):
            relay = relay + rsb[b, p].astype(F32)
        zb[b] = relay.astype(BF16)
        kept.append(relay[0:TILE])
        for o in outer:
            to_peer(
                zb.at[b, rows_at(o, 1)], rsc.at[b, rows_at(o, 1)], sc.at[0], rc.at[b], o * I
            ).start()

    res_x.wait()
    att_all.wait_send()
    trow = lax.broadcasted_iota(jnp.int32, (T, half), 0)
    base = jnp.where(trow // S == c, resb[:, mine], resp[...])
    table = tts[...].astype(BF16)

    x_x = []

    def dispatch(k, total):
        cols = slice(k * step, (k + 1) * step)
        hidden = base[:, cols] + jnp.concatenate([total[:T], total[T:]], axis=1)
        hs[:, cols] = hidden
        picked = lax.dot_general(
            table, hidden.astype(BF16), (((0,), (0,)), ((), ())), preferred_element_type=F32
        )
        for m in range(E):
            xb[k, m] = picked[m * cap:(m + 1) * cap].astype(BF16)
        for m in far_first:
            to_peer(xb.at[k, m], xr.at[k, m], sx.at[0], rx.at[k], m).start()
        xr[k, 0] = picked[0:cap].astype(BF16)
        x_x.append(whole(xr.at[k, pl.ds(1, E - 1)], sx.at[0], rx.at[k]))

    for k in range(direct):
        a_x[k].wait_recv()
        total = ys[k, 0:TILE, :].astype(F32)
        for m in range(1, E):
            total = total + rsa[k, m * TILE:(m + 1) * TILE, :].astype(F32)
        dispatch(k, total)
    for b in range(C - direct):
        c_x[b].wait_recv()
        total = kept[b]
        for o in range(1, O):
            total = total + rsc[b, o * TILE:(o + 1) * TILE, :].astype(F32)
        dispatch(direct + b, total)

    for cp in wcopies[2:]:
        cp.wait()
    wg_x.wait()
    wu_x.wait()
    wd_x.wait()
    whole(rsa.at[:, rows_at(1, E - 1)], sa.at[0], ra.at[0]).wait_send()
    whole(rsb.at[:, pl.ds(1, I - 1)], sb.at[0], rb.at[0]).wait_send()
    whole(rsc.at[:, rows_at(1, O - 1)], sc.at[0], rc.at[0]).wait_send()
    rows = E * cap
    gain = gain_ref[mine].astype(F32).reshape(1, half)
    square = jnp.zeros((rows, 1), F32)
    F = 2 * FH
    gates, ups = slice(128, 128 + F), slice(128 + F, 128 + 2 * F)
    for k in range(C):
        x_x[k].wait_recv()
        feats = slice(k * step, (k + 1) * step)
        part = xr[k].astype(F32).reshape(rows, step)
        square = square + jnp.sum(part * part, axis=1, keepdims=True)
        xs[:, feats] = (part * gain[:, feats]).astype(BF16)
        if k == 0:
            gus[:, gates] = dot(xs[:, feats], wg[feats, :])
        else:
            gus[:, gates] += dot(xs[:, feats], wg[feats, :])
        if k == C - 1:
            gus[:, 0:128] = jnp.broadcast_to(square, (rows, 128))
            first = pl.ds(0, 128 + F)
            g_x = beside(gus.at[:, first], gur.at[:, first], 5)
            g_x.start()
        if k == 0:
            gus[:, ups] = dot(xs[:, feats], wu[feats, :])
        else:
            gus[:, ups] += dot(xs[:, feats], wu[feats, :])
    second = pl.ds(128 + F, F)
    u_x = beside(gus.at[:, second], gur.at[:, second], 6)
    u_x.start()
    g_x.wait()
    scale = lax.rsqrt((gus[:, 0:1] + gur[:, 0:1]) / D + 1e-06)
    gate = (gus[:, 128:128 + F] + gur[:, 128:128 + F]) * scale
    gate = gate / (1.0 + jnp.exp(-gate))
    u_x.wait()
    up = (gus[:, 128 + F:128 + 2 * F] + gur[:, 128 + F:128 + 2 * F]) * scale
    hid[...] = (gate * up).astype(BF16)

    stepz = half // Z
    z_x = []
    for k in range(Z):
        o = dot(hid[...], wd[:, k * stepz:(k + 1) * stepz])
        for m in range(E):
            zs[k, m] = o[m * cap:(m + 1) * cap].astype(BF16)
        for m in far_first:
            to_peer(zs.at[k, m], zr.at[k, m], sz.at[0], rz.at[k], m).start()
        zr[k, 0] = o[0:cap].astype(BF16)
        z_x.append(whole(zr.at[k, pl.ds(1, E - 1)], sz.at[0], rz.at[k]))

    whole(xr.at[:, pl.ds(1, E - 1)], sx.at[0], rx.at[0]).wait_send()
    wh = whi[...].astype(BF16)
    wl = wlo[...].astype(BF16)
    own = c == 0
    for k in range(Z):
        z_x[k].wait_recv()
        part = zr[k].astype(F32).reshape(rows, stepz).astype(BF16)
        cols = slice(k * stepz, (k + 1) * stepz)
        updated = hs[:, cols] + dot(wh, part) + dot(wl, part)
        ub[:, cols] = updated
        beside(ub.at[:, pl.ds(k * stepz, stepz)], up_.at[:, pl.ds(k * stepz, stepz)], 7).start()
        at = pl.ds(pl.multiple_of(c * half + k * stepz, stepz), stepz)
        out_ref[:, at] = jnp.where(own, updated[:S], updated[S:]).astype(BF16)
    whole(zr.at[:, pl.ds(1, E - 1)], sz.at[0], rz.at[0]).wait_send()
    beside(ub, up_, 7).wait()
    got = up_[...]
    out_ref[:, other] = jnp.where(own, got[:S], got[S:]).astype(BF16)


def on_device(
    queries, token_keys, token_values, stored_keys, stored_values, kv_len, residual, out_weight,
    norm_gain, expert_ids, route_weight, w_gate, w_up, w_down,
):
    E = lax.axis_size("expert")
    N = 2 * E
    I = 1 << ((E.bit_length() - 1) // 2)
    O = E // I
    S, features = queries.shape
    T = 2 * S
    L = stored_keys.shape[1]
    KW = token_keys.shape[1]
    D = residual.shape[1]
    half = D // 2
    topk = expert_ids.shape[1]
    FH = w_gate.shape[2]
    cap = max(2, -(-(T * topk) // E))
    C = CHUNKS
    Z = RETURNS
    A = C // 2
    B = C - A
    step = half // C
    lanes = step // 2
    orow = out_weight.shape[0]
    hbm = pl.BlockSpec(memory_space=pltpu.HBM)
    V = pltpu.VMEM
    dma = pltpu.SemaphoreType.DMA
    wout = 128 + 4 * FH
    scratch = [
        V((S, features), BF16), V((S, KW), BF16), V((S, KW), BF16), pltpu.SMEM((S,), jnp.int32),
        V((S, D), BF16), V((D,), BF16), V(expert_ids.shape, jnp.int32), V(route_weight.shape, F32),
        V((S, L, KW), BF16), V((S, L, KW), BF16),
        V((orow, half), BF16), V((2 * orow, half), BF16),
        V((half, 2 * FH), BF16), V((half, 2 * FH), BF16), V((2 * FH, half), BF16),
        V((S * features // HEAD_WIDTH, HEAD_WIDTH), F32), V((8, KW), F32), V((8, KW), F32),
        V((E * TILE, HEAD_WIDTH), F32), V((E * TILE, HEAD_WIDTH), BF16),
        V((N * TILE, HEAD_WIDTH), BF16), V((N * S, 2 * orow), BF16),
        V((C, E * TILE, lanes), BF16), V((A, E * TILE, lanes), BF16),
        V((B, I, O * TILE, lanes), BF16), V((B, O * TILE, lanes), BF16), V((B, O * TILE, lanes), BF16),
        V((T, D), F32), V((T, half), F32), V((T, half), F32),
        V((T, E * cap), F32), V((T, E * cap), F32), V((T, E * cap), F32),
        V((C, E, cap, step), BF16), V((C, E, cap, step), BF16), V((E * cap, half), BF16),
        V((E * cap, wout), F32), V((E * cap, wout), F32), V((E * cap, 2 * FH), BF16),
        V((Z, E, cap, half // Z), BF16), V((Z, E, cap, half // Z), BF16),
        V((T, half), F32), V((T, half), F32),
        dma((8,)), dma((2,)), dma((5,)), dma((8,)), dma((8,)),
        dma((1,)), dma((1,)), dma((1,)), dma((A,)), dma((1,)), dma((B,)), dma((1,)), dma((B,)),
        dma((1,)), dma((C,)), dma((1,)), dma((Z,)),
    ]
    return pl.pallas_call(
        functools.partial(kernel, E, I, cap, C, A, Z),
        out_shape=pltpu.VMEM((S, D), BF16),
        in_specs=[hbm] * 14,
        out_specs=pl.BlockSpec(memory_space=pltpu.VMEM),
        scratch_shapes=scratch,
        compiler_params=pltpu.CompilerParams(
            collective_id=0, has_side_effects=True, vmem_limit_bytes=66977792
        ),
    )(
        queries, token_keys, token_values, kv_len, residual, norm_gain, expert_ids,
        route_weight, stored_keys, stored_values, out_weight, w_gate, w_up, w_down,
    )


def solution(mesh):
    rows = P(("groups", "expert", "replica"), None)
    cube = P(("groups", "expert", "replica"), None, None)
    in_specs = (
        rows, rows, rows, cube, cube, P(("groups", "expert", "replica")), rows,
        P(("expert", "replica"), None), P(), P(("groups", "expert"), None),
        P(("groups", "expert"), None), P("expert", None, "replica"),
        P("expert", None, "replica"), P("expert", "replica", None),
    )
    return jax.shard_map(
        on_device, mesh=mesh, in_specs=in_specs, out_specs=rows, check_vma=False
    )
```

```python
import functools
import math

import jax
import jax.numpy as jnp
from jax import lax
from jax.experimental import pallas as pl
from jax.experimental.pallas import tpu as pltpu
from jax.sharding import PartitionSpec as P

HEAD_WIDTH = 128
TILE = 16
CHUNKS = 4
RETURNS = 2
MESH = pl.DeviceIdType.MESH
F32 = jnp.float32
BF16 = jnp.bfloat16


def permutation(size, source):
    a = lax.broadcasted_iota(jnp.int32, (size, 8 * TILE), 0)
    b = lax.broadcasted_iota(jnp.int32, (size, 8 * TILE), 1)
    return jnp.where(b == source(a), 1.0, 0.0).astype(BF16)


def heads_out(hpc, S):
    return permutation(
        8 * hpc * S,
        lambda a: ((a // S) % 8) * TILE + (a % S) * hpc + a // (8 * S),
    )


def dot(a, b):
    return jnp.dot(a, b, preferred_element_type=F32)


def kernel(
    E, I, cap, C, direct, Z,
    q_hbm, tk_hbm, tv_hbm, kv_hbm, res_hbm, gain_hbm, ids_hbm, rw_hbm,
    k_hbm, v_hbm, ow_hbm, wg_hbm, wu_hbm, wd_hbm,
    out_ref,
    q_ref, tk_ref, tv_ref, kv_ref, res_ref, gain_ref, ids_ref, rw_ref,
    kb, vb, owo, ow, wg, wu, wd,
    qs, tks, tvs, attf, att, ratt, asm,
    ys, rsa, rsb, zb, rsc,
    resb, resp, hs, tts, whi, wlo,
    xb, xr, xs, gus, gur, hid, zs, zr, ub, up_,
    isem, ksem, wsem, psend, precv,
    s1, r1, sa, ra, sb, rb, sc, rc, sx, rx, sz, rz,
):
    N = 2 * E
    O = E // I
    bits = E.bit_length() - 1
    e_me = lax.axis_index("expert")
    c = lax.axis_index("replica")
    rank = e_me * 2 + c
    S = q_ref.shape[0]
    T = 2 * S
    heads = q_ref.shape[1] // HEAD_WIDTH
    G = tk_ref.shape[1] // HEAD_WIDTH
    width = heads // G
    L = k_hbm.shape[1]
    D = res_ref.shape[1]
    half = D // 2
    hpc = heads // E
    step = half // C
    FH = wg_hbm.shape[2]
    orow = ow_hbm.shape[0]
    drow = wd_hbm.shape[1]
    mine = pl.ds(pl.multiple_of(c * half, half), half)
    other = pl.ds(pl.multiple_of((1 - c) * half, half), half)
    omine = pl.ds(pl.multiple_of(c * orow, orow), orow)
    dmine = pl.ds(pl.multiple_of(c * drow, drow), drow)
    fmine = pl.ds(pl.multiple_of(c * FH, FH), FH)

    place = []
    for k in range(bits):
        bit = lax.rem(lax.div(e_me, 1 << k), 2)
        place.append((bit * (1 << k), (1 - bit) * (1 << k)))

    def expert_at(mask):
        return functools.reduce(lambda a, b: a + b, [place[k][(mask >> k) & 1] for k in range(bits)])

    peer = [expert_at(m) for m in range(E)]
    side = [c, 1 - c]
    order = {m: (m % I) * O + m // I for m in range(E)}

    small = [
        pltpu.make_async_copy(src, dst, isem.at[k])
        for k, (src, dst) in enumerate((
            (q_hbm, q_ref), (tk_hbm, tk_ref), (tv_hbm, tv_ref), (kv_hbm, kv_ref),
            (res_hbm, res_ref), (gain_hbm, gain_ref), (ids_hbm, ids_ref), (rw_hbm, rw_ref),
        ))
    ]
    k_copy = pltpu.make_async_copy(k_hbm, kb, ksem.at[0])
    v_copy = pltpu.make_async_copy(v_hbm, vb, ksem.at[1])
    wcopies = [
        pltpu.make_async_copy(ow_hbm.at[:, other], owo, wsem.at[0]),
        pltpu.make_async_copy(ow_hbm.at[:, mine], ow.at[omine], wsem.at[1]),
        pltpu.make_async_copy(wg_hbm.at[0, mine], wg.at[:, fmine], wsem.at[2]),
        pltpu.make_async_copy(wu_hbm.at[0, mine], wu.at[:, fmine], wsem.at[3]),
        pltpu.make_async_copy(wd_hbm.at[0, :, mine], wd.at[dmine], wsem.at[4]),
    ]
    for cp in small[:4] + [k_copy, v_copy]:
        cp.start()
    barrier = pltpu.get_barrier_semaphore()
    for m in range(E - 1, -1, -1):
        for k in (0, 1):
            if m or k:
                pl.semaphore_signal(
                    barrier, inc=1,
                    device_id={"expert": peer[m], "replica": side[k]}, device_id_type=MESH,
                )
    for cp in small[4:]:
        cp.start()

    for cp in small[:4]:
        cp.wait()
    qf = q_ref[...].astype(F32)
    for h in range(heads):
        qs[pl.ds(S * h, S), :] = qf[:, h * HEAD_WIDTH:(h + 1) * HEAD_WIDTH]
    tks[0:S, :] = tk_ref[...].astype(F32)
    tvs[0:S, :] = tv_ref[...].astype(F32)
    if hpc * S < TILE:
        attf[...] = jnp.zeros_like(attf)
    inv_root = 1.0 / math.sqrt(HEAD_WIDTH)
    group = lax.broadcasted_iota(jnp.int32, (heads, HEAD_WIDTH), 0) // width
    col = lax.broadcasted_iota(jnp.int32, (heads, L), 1)

    def by_head(ref, b):
        return jnp.concatenate([
            jnp.broadcast_to(ref[b:b + 1, g * HEAD_WIDTH:(g + 1) * HEAD_WIDTH], (width, HEAD_WIDTH))
            for g in range(G)
        ], axis=0)

    rows_q = []
    fresh = []
    for b in range(S):
        qb = qs[pl.ds(b, heads, stride=S), :]
        rows_q.append(jnp.concatenate(
            [jnp.where(group == g, qb, 0.0).astype(BF16) for g in range(G)], axis=1
        ))
        fresh.append(jnp.sum(qb * by_head(tks, b), axis=1, keepdims=True) * inv_root)
    k_copy.wait()
    probs = []
    fprobs = []
    for b in range(S):
        score = lax.dot_general(
            rows_q[b], kb[b], (((1,), (1,)), ((), ())),
            preferred_element_type=F32,
        ) * inv_root
        score = jnp.where(col < kv_ref[b], score, -jnp.inf)
        top = jnp.maximum(jnp.max(score, axis=1, keepdims=True), fresh[b])
        ex = jnp.exp(score - top)
        fex = jnp.exp(fresh[b] - top)
        inv = 1.0 / (jnp.sum(ex, axis=1, keepdims=True) + fex)
        probs.append((ex * inv).astype(BF16))
        fprobs.append((fex * inv).astype(BF16).astype(F32))
    v_copy.wait()
    for cp in wcopies:
        cp.start()
    for b in range(S):
        o = dot(probs[b], vb[b])
        o = jnp.concatenate([
            o[g * width:(g + 1) * width, g * HEAD_WIDTH:(g + 1) * HEAD_WIDTH] for g in range(G)
        ], axis=0)
        o = o + fprobs[b] * by_head(tvs, b)
        for j in range(E):
            attf[j * TILE + b * hpc:j * TILE + (b + 1) * hpc, :] = o[j * hpc:(j + 1) * hpc]
    att[...] = attf[...].astype(BF16)

    pl.semaphore_wait(barrier, N - 1)

    def rows_at(start, count):
        return pl.ds(pl.multiple_of(start * TILE, TILE), count * TILE)

    def att_copy(m, k):
        return pltpu.make_async_remote_copy(
            src_ref=att.at[rows_at(peer[m], 1)], dst_ref=ratt.at[rows_at(2 * order[m] + c, 1)],
            send_sem=s1.at[0], recv_sem=r1.at[0],
            device_id={"expert": peer[m], "replica": k if m else side[k]}, device_id_type=MESH,
        )

    def to_peer(src, dst, send, recv, m):
        return pltpu.make_async_remote_copy(
            src_ref=src, dst_ref=dst, send_sem=send, recv_sem=recv,
            device_id={"expert": peer[m], "replica": c}, device_id_type=MESH,
        )

    def beside(src, dst, k):
        return pltpu.make_async_remote_copy(
            src_ref=src, dst_ref=dst, send_sem=psend.at[k], recv_sem=precv.at[k],
            device_id={"expert": e_me, "replica": 1 - c}, device_id_type=MESH,
        )

    def whole(ref, send, recv):
        return to_peer(ref, ref, send, recv, E - 1)

    far_first = range(E - 1, 0, -1)
    att_x = [att_copy(m, k) for m in far_first for k in (0, 1)] + [att_copy(0, 1)]
    for cp in att_x:
        cp.start()
    att_all = whole(ratt.at[rows_at(0, N - 1)], s1.at[0], r1.at[0])
    wcopies[0].wait()
    wg_x = beside(wg_hbm.at[0, other], wg.at[:, fmine], 2)
    wu_x = beside(wu_hbm.at[0, other], wu.at[:, fmine], 3)
    wd_x = beside(wd_hbm.at[0, :, other], wd.at[dmine], 4)
    ow_x = beside(owo, ow.at[omine], 0)
    ow_x.start()
    for cp in (wg_x, wu_x, wd_x):
        cp.start()
    for cp in small[4:]:
        cp.wait()
    ratt[rows_at(c, 1)] = att[rows_at(e_me, 1)]
    for rep in range(8 // S):
        resb[pl.ds(rep * S, S), :] = res_ref[...].astype(F32)
    res_x = beside(resb.at[:, other], resp, 1)
    res_x.start()

    lanes_all = E * cap
    lane = lax.broadcasted_iota(jnp.int32, (T, lanes_all), 1)
    tok = lax.broadcasted_iota(jnp.int32, (T, lanes_all), 0)
    lm = lane // cap
    le = jnp.zeros((T, lanes_all), jnp.int32)
    for k in range(bits):
        flip = (lm // (1 << k)) % 2
        le = le + jnp.where(flip == 1, place[k][1], place[k][0])
    ls = lane % cap
    ids = ids_ref[...]
    rw = rw_ref[...]
    mix = rw / jnp.sum(rw, axis=1, keepdims=True)
    named = jnp.zeros((T, lanes_all), F32)
    weight = jnp.zeros((T, lanes_all), F32)
    for k in range(ids.shape[1]):
        hit = ids[:, k:k + 1] == le
        named = named + jnp.where(hit, 1.0, 0.0)
        weight = weight + jnp.where(hit, mix[:, k:k + 1], 0.0)
    before = jnp.zeros((T, lanes_all), F32)
    for t in range(T - 1):
        before = before + jnp.where(tok > t, named[t:t + 1, :], 0.0)
    chosen = jnp.where(before == ls.astype(F32), named, 0.0)
    weight = weight * chosen
    high = weight.astype(BF16).astype(F32)
    low = weight - high
    tts[...] = chosen
    whi[...] = high
    wlo[...] = low

    wcopies[1].wait()
    ow_x.wait()
    att_all.wait_recv()

    pa = heads_out(hpc, S)
    for grp in range(N // 8):
        blk = dot(pa, ratt[grp * 8 * TILE:(grp + 1) * 8 * TILE, :]).astype(BF16)
        for h in range(hpc):
            asm[grp * 8 * S:(grp + 1) * 8 * S, h * HEAD_WIDTH:(h + 1) * HEAD_WIDTH] = (
                blk[h * 8 * S:(h + 1) * 8 * S]
            )
    lanes = step // 2
    inner = range(I - 1, 0, -1)
    outer = range(O - 1, 0, -1)
    for k in [*range(direct, C), *range(direct)]:
        y = [
            dot(asm[...], ow[:, k * step + j * lanes:k * step + (j + 1) * lanes]) for j in (0, 1)
        ]
        both = jnp.concatenate([v.reshape(E, T, lanes) for v in y], axis=1)
        ys[k] = both.reshape(E * TILE, lanes).astype(BF16)
        if k < direct:
            for m in far_first:
                to_peer(
                    ys.at[k, rows_at(order[m], 1)], rsa.at[k, rows_at(order[m], 1)],
                    sa.at[0], ra.at[k], m,
                ).start()
        else:
            b = k - direct
            for p in inner:
                to_peer(
                    ys.at[k, rows_at(p * O, O)], rsb.at[b, p], sb.at[0], rb.at[b], p
                ).start()
    a_x = [whole(rsa.at[k, rows_at(1, E - 1)], sa.at[0], ra.at[k]) for k in range(direct)]
    b_x = [whole(rsb.at[b, pl.ds(1, I - 1)], sb.at[0], rb.at[b]) for b in range(C - direct)]
    c_x = [whole(rsc.at[b, rows_at(1, O - 1)], sc.at[0], rc.at[b]) for b in range(C - direct)]
    kept = []
    for b in range(C - direct):
        b_x[b].wait_recv()
        relay = ys[direct + b, 0:O * TILE, :].astype(F32)
        for p in range(1, I):
            relay = relay + rsb[b, p].astype(F32)
        zb[b] = relay.astype(BF16)
        kept.append(relay[0:TILE])
        for o in outer:
            to_peer(
                zb.at[b, rows_at(o, 1)], rsc.at[b, rows_at(o, 1)], sc.at[0], rc.at[b], o * I
            ).start()

    res_x.wait()
    att_all.wait_send()
    trow = lax.broadcasted_iota(jnp.int32, (T, half), 0)
    base = jnp.where(trow // S == c, resb[:, mine], resp[...])
    table = tts[...].astype(BF16)

    x_x = []

    def dispatch(k, total):
        cols = slice(k * step, (k + 1) * step)
        hidden = base[:, cols] + jnp.concatenate([total[:T], total[T:]], axis=1)
        hs[:, cols] = hidden
        picked = lax.dot_general(
            table, hidden.astype(BF16), (((0,), (0,)), ((), ())), preferred_element_type=F32
        )
        for m in range(E):
            xb[k, m] = picked[m * cap:(m + 1) * cap].astype(BF16)
        for m in far_first:
            to_peer(xb.at[k, m], xr.at[k, m], sx.at[0], rx.at[k], m).start()
        xr[k, 0] = picked[0:cap].astype(BF16)
        x_x.append(whole(xr.at[k, pl.ds(1, E - 1)], sx.at[0], rx.at[k]))

    for k in range(direct):
        a_x[k].wait_recv()
        total = ys[k, 0:TILE, :].astype(F32)
        for m in range(1, E):
            total = total + rsa[k, m * TILE:(m + 1) * TILE, :].astype(F32)
        dispatch(k, total)
    for b in range(C - direct):
        c_x[b].wait_recv()
        total = kept[b]
        for o in range(1, O):
            total = total + rsc[b, o * TILE:(o + 1) * TILE, :].astype(F32)
        dispatch(direct + b, total)

    for cp in wcopies[2:]:
        cp.wait()
    wg_x.wait()
    wu_x.wait()
    wd_x.wait()
    whole(rsa.at[:, rows_at(1, E - 1)], sa.at[0], ra.at[0]).wait_send()
    whole(rsb.at[:, pl.ds(1, I - 1)], sb.at[0], rb.at[0]).wait_send()
    whole(rsc.at[:, rows_at(1, O - 1)], sc.at[0], rc.at[0]).wait_send()
    rows = E * cap
    gain = gain_ref[mine].astype(F32).reshape(1, half)
    square = jnp.zeros((rows, 1), F32)
    F = 2 * FH
    gates, ups = slice(128, 128 + F), slice(128 + F, 128 + 2 * F)
    for k in range(C):
        x_x[k].wait_recv()
        feats = slice(k * step, (k + 1) * step)
        part = xr[k].astype(F32).reshape(rows, step)
        square = square + jnp.sum(part * part, axis=1, keepdims=True)
        xs[:, feats] = (part * gain[:, feats]).astype(BF16)
        if k == 0:
            gus[:, gates] = dot(xs[:, feats], wg[feats, :])
        else:
            gus[:, gates] += dot(xs[:, feats], wg[feats, :])
        if k == C - 1:
            gus[:, 0:128] = jnp.broadcast_to(square, (rows, 128))
            first = pl.ds(0, 128 + F)
            g_x = beside(gus.at[:, first], gur.at[:, first], 5)
            g_x.start()
        if k == 0:
            gus[:, ups] = dot(xs[:, feats], wu[feats, :])
        else:
            gus[:, ups] += dot(xs[:, feats], wu[feats, :])
    second = pl.ds(128 + F, F)
    u_x = beside(gus.at[:, second], gur.at[:, second], 6)
    u_x.start()
    g_x.wait()
    scale = lax.rsqrt((gus[:, 0:1] + gur[:, 0:1]) / D + 1e-06)
    gate = (gus[:, 128:128 + F] + gur[:, 128:128 + F]) * scale
    gate = gate / (1.0 + jnp.exp(-gate))
    u_x.wait()
    up = (gus[:, 128 + F:128 + 2 * F] + gur[:, 128 + F:128 + 2 * F]) * scale
    hid[...] = (gate * up).astype(BF16)

    stepz = half // Z
    z_x = []
    for k in range(Z):
        o = dot(hid[...], wd[:, k * stepz:(k + 1) * stepz])
        for m in range(E):
            zs[k, m] = o[m * cap:(m + 1) * cap].astype(BF16)
        for m in far_first:
            to_peer(zs.at[k, m], zr.at[k, m], sz.at[0], rz.at[k], m).start()
        zr[k, 0] = o[0:cap].astype(BF16)
        z_x.append(whole(zr.at[k, pl.ds(1, E - 1)], sz.at[0], rz.at[k]))

    whole(xr.at[:, pl.ds(1, E - 1)], sx.at[0], rx.at[0]).wait_send()
    wh = whi[...].astype(BF16)
    wl = wlo[...].astype(BF16)
    own = c == 0
    for k in range(Z):
        z_x[k].wait_recv()
        part = zr[k].astype(F32).reshape(rows, stepz).astype(BF16)
        cols = slice(k * stepz, (k + 1) * stepz)
        updated = hs[:, cols] + dot(wh, part) + dot(wl, part)
        ub[:, cols] = updated
        beside(ub.at[:, pl.ds(k * stepz, stepz)], up_.at[:, pl.ds(k * stepz, stepz)], 7).start()
        at = pl.ds(pl.multiple_of(c * half + k * stepz, stepz), stepz)
        out_ref[:, at] = jnp.where(own, updated[:S], updated[S:]).astype(BF16)
    whole(zr.at[:, pl.ds(1, E - 1)], sz.at[0], rz.at[0]).wait_send()
    beside(ub, up_, 7).wait()
    got = up_[...]
    out_ref[:, other] = jnp.where(own, got[:S], got[S:]).astype(BF16)


def on_device(
    queries, token_keys, token_values, stored_keys, stored_values, kv_len, residual, out_weight,
    norm_gain, expert_ids, route_weight, w_gate, w_up, w_down,
):
    E = lax.axis_size("expert")
    N = 2 * E
    I = 1 << ((E.bit_length() - 1) // 2)
    O = E // I
    S, features = queries.shape
    T = 2 * S
    L = stored_keys.shape[1]
    KW = token_keys.shape[1]
    D = residual.shape[1]
    half = D // 2
    topk = expert_ids.shape[1]
    FH = w_gate.shape[2]
    cap = max(2, -(-(T * topk) // E))
    C = CHUNKS
    Z = RETURNS
    A = C // 2
    B = C - A
    step = half // C
    lanes = step // 2
    orow = out_weight.shape[0]
    hbm = pl.BlockSpec(memory_space=pltpu.HBM)
    V = pltpu.VMEM
    dma = pltpu.SemaphoreType.DMA
    wout = 128 + 4 * FH
    scratch = [
        V((S, features), BF16), V((S, KW), BF16), V((S, KW), BF16), pltpu.SMEM((S,), jnp.int32),
        V((S, D), BF16), V((D,), BF16), V(expert_ids.shape, jnp.int32), V(route_weight.shape, F32),
        V((S, L, KW), BF16), V((S, L, KW), BF16),
        V((orow, half), BF16), V((2 * orow, half), BF16),
        V((half, 2 * FH), BF16), V((half, 2 * FH), BF16), V((2 * FH, half), BF16),
        V((S * features // HEAD_WIDTH, HEAD_WIDTH), F32), V((8, KW), F32), V((8, KW), F32),
        V((E * TILE, HEAD_WIDTH), F32), V((E * TILE, HEAD_WIDTH), BF16),
        V((N * TILE, HEAD_WIDTH), BF16), V((N * S, 2 * orow), BF16),
        V((C, E * TILE, lanes), BF16), V((A, E * TILE, lanes), BF16),
        V((B, I, O * TILE, lanes), BF16), V((B, O * TILE, lanes), BF16), V((B, O * TILE, lanes), BF16),
        V((T, D), F32), V((T, half), F32), V((T, half), F32),
        V((T, E * cap), F32), V((T, E * cap), F32), V((T, E * cap), F32),
        V((C, E, cap, step), BF16), V((C, E, cap, step), BF16), V((E * cap, half), BF16),
        V((E * cap, wout), F32), V((E * cap, wout), F32), V((E * cap, 2 * FH), BF16),
        V((Z, E, cap, half // Z), BF16), V((Z, E, cap, half // Z), BF16),
        V((T, half), F32), V((T, half), F32),
        dma((8,)), dma((2,)), dma((5,)), dma((8,)), dma((8,)),
        dma((1,)), dma((1,)), dma((1,)), dma((A,)), dma((1,)), dma((B,)), dma((1,)), dma((B,)),
        dma((1,)), dma((C,)), dma((1,)), dma((Z,)),
    ]
    return pl.pallas_call(
        functools.partial(kernel, E, I, cap, C, A, Z),
        out_shape=pltpu.VMEM((S, D), BF16),
        in_specs=[hbm] * 14,
        out_specs=pl.BlockSpec(memory_space=pltpu.VMEM),
        scratch_shapes=scratch,
        compiler_params=pltpu.CompilerParams(
            collective_id=0, has_side_effects=True, vmem_limit_bytes=66977792
        ),
    )(
        queries, token_keys, token_values, kv_len, residual, norm_gain, expert_ids,
        route_weight, stored_keys, stored_values, out_weight, w_gate, w_up, w_down,
    )


def solution(mesh):
    rows = P(("groups", "expert", "replica"), None)
    cube = P(("groups", "expert", "replica"), None, None)
    in_specs = (
        rows, rows, rows, cube, cube, P(("groups", "expert", "replica")), rows,
        P(("expert", "replica"), None), P(), P(("groups", "expert"), None),
        P(("groups", "expert"), None), P("expert", None, "replica"),
        P("expert", None, "replica"), P("expert", "replica", None),
    )
    return jax.shard_map(
        on_device, mesh=mesh, in_specs=in_specs, out_specs=rows, check_vma=False
    )
```
